512 devices in a mesh: lat: 64 (over z, y), lon: 8 (over x, core).
Axes of the slice: x: 4, y: 8, z: 8, core: 2. Of those that a mesh axis runs over, the one named last changes fastest.
Arguments:
- fields: bfloat16 [8192, 8, 1024], P('lat', 'lon'), may hold values from -6 to 6
- proj_x: bfloat16 [1024, 1024], P('lon'), may hold values from -0.1875 to 0.1875
- proj_z: bfloat16 [1024, 1024], P('lon'), may hold values from -0.1875 to 0.1875
- proj_bc: bfloat16 [1024, 128], P('lon'), may hold values from -0.1875 to 0.1875
- proj_dt: bfloat16 [1024, 16], P('lon'), may hold values from -1 to 1
- conv_x: float32 [4, 1024], replicated, may hold values from -3 to 3
- conv_bc: float32 [4, 128], replicated, may hold values from -3 to 3
- dt_bias: float32 [16], replicated, may hold values from -1 to 0.5
- log_rate: float32 [16], replicated, may hold values from -12 to -2.7
- norm_gain: float32 [1024], replicated, may hold values from 0.1 to 1.9
- proj_out: bfloat16 [1024, 1024], P('lon'), may hold values from -0.1875 to 0.1875
Outputs:
- mixer_out: bfloat16 [8192, 8, 1024], P('lat', 'lon')
The draws below stay inside these ranges and needn't reach their ends.
All inputs are finite; a program needn't handle non-finite values.
Results may differ from the reference program's by a relative error of at most 0.012.
Values may be sent and summed in bfloat16 or wider, within the bound.
No kernel may reach another device: no remote copies, remote signals or barrier semaphores. Data moves between devices by JAX's collectives and lax.ppermute only.
A program may use at most 64 MiB of HBM per device.

```python
import jax
import jax.numpy as jnp
from jax import lax

D = 1024
HEADS = 16
HEAD_DIM = 64
STATE = 64
KERNEL = 4
LAT_DEV = 128
INNER = 1024
LAT = 8192
LON = 8


def shared_direction(key):
    base_key = jax.random.fold_in(key, 101)
    key_dir, key_size, key_sign = jax.random.split(base_key, 3)
    direction = jax.random.normal(key_dir, (D,), jnp.float32)
    direction = direction / jnp.sqrt(jnp.sum(direction * direction))
    head_size = jax.random.uniform(key_size, (HEADS,), jnp.float32, 0.4, 0.7)
    head_sign = jnp.where(jax.random.uniform(key_sign, (HEADS,), jnp.float32) < 0.5, -1.0, 1.0)
    return (direction, head_size * head_sign)


def draw_fields(key, part):
    direction, head_weight = shared_direction(key)
    own_key = jax.random.fold_in(key, 202)
    key_noise, key_level, key_jitter = jax.random.split(own_key, 3)
    segment = max(1, 3 * LAT_DEV // 2)
    level_count = LAT // segment + 1
    noise = jax.random.normal(key_noise, (LAT, LON, D), jnp.float32)
    levels = jax.random.uniform(key_level, (level_count,), jnp.float32, -3.5, 3.5)
    row_level = levels[jnp.arange(LAT) // segment]
    along = row_level + 0.5 * jax.random.normal(key_jitter, (LAT,), jnp.float32)
    values = noise + along[:, None, None] * direction[None, None, :]
    return jnp.clip(values, -6.0, 6.0).astype(jnp.bfloat16)


def draw_proj_dt(key, part):
    direction, head_weight = shared_direction(key)
    own_key = jax.random.fold_in(key, 303)
    base = jax.random.normal(own_key, (D, HEADS), jnp.float32) / jnp.sqrt(16.0 * D)
    values = base + direction[:, None] * head_weight[None, :]
    return jnp.clip(values, -1.0, 1.0).astype(jnp.bfloat16)


def draw_log_rate(key, part):
    key_slow, key_pick, key_long, key_short = jax.random.split(jax.random.fold_in(key, 17), 4)
    slow_share = 0.5
    slow_heads = jax.random.uniform(key_slow, (HEADS,), jnp.float32) < slow_share
    picked = jnp.arange(HEADS) == jax.random.randint(key_pick, (), 0, HEADS)
    slow_heads = jnp.logical_or(slow_heads, picked)
    long_reach = jnp.exp(jax.random.uniform(key_long, (HEADS,), jnp.float32, jnp.log(0.2), jnp.log(1.0)))
    short_reach = jnp.exp(jax.random.uniform(key_short, (HEADS,), jnp.float32, jnp.log(25.0), jnp.log(50.0)))
    rates = jnp.where(slow_heads, long_reach / (0.6 * LAT), 1.0 / (0.6 * short_reach))
    return jnp.log(rates).astype(jnp.float32)


def block_levels(stream_key, shape, cuts, least, high):
    gain = 1.0
    for dim, shards_of in cuts:
        heights = jax.random.uniform(jax.random.fold_in(jax.random.fold_in(stream_key, 6), dim), (shards_of,), jnp.float32, least / len(cuts), high / len(cuts))
        gain = gain * jnp.repeat(jnp.exp(heights), shape[dim] // shards_of).reshape((-1,) + (1,) * (len(shape) - 1 - dim))
    return gain


def normal_values(stream_key, shape, scale, limit, cuts=(), kind=jnp.bfloat16):
    values = jax.random.normal(stream_key, shape, jnp.float32) * scale
    if len(cuts) > 0:
        values = block_levels(stream_key, shape, cuts, -0.22, 0.18) * values
    return jnp.clip(values, min=-limit, max=limit).astype(kind)


def setup_inputs(seed: int = 0) -> dict:
    seeds = jax.random.split(jax.random.key(seed), 12)
    fields = draw_fields(jax.random.fold_in(seeds[11], 71), 0)
    proj_x = normal_values(seeds[1], (D, INNER), D ** -0.5, 0.1875, ((0, 8),))
    proj_z = normal_values(seeds[2], (D, INNER), D ** -0.5, 0.1875, ((0, 8),))
    proj_bc = normal_values(seeds[3], (D, 2 * STATE), D ** -0.5, 0.1875, ((0, 8),))
    proj_dt = draw_proj_dt(jax.random.fold_in(seeds[11], 71), 0)
    conv_x = normal_values(seeds[5], (KERNEL, INNER), KERNEL ** -0.5, 3.0, (), jnp.float32)
    conv_bc = normal_values(seeds[6], (KERNEL, 2 * STATE), KERNEL ** -0.5, 3.0, (), jnp.float32)
    dt_bias = jnp.clip(jax.random.uniform(seeds[7], (HEADS,), jnp.float32, -1.0, 0.5), -1.0, 0.5)
    log_rate = draw_log_rate(jax.random.fold_in(seeds[11], 71), 0)
    norm_gain = jnp.clip(1.0 + 0.18 * jax.random.normal(seeds[9], (INNER,), jnp.float32), 0.1, 1.9)
    proj_out = normal_values(seeds[10], (INNER, D), INNER ** -0.5, 0.1875, ((0, 8),))
    return {"fields": fields, "proj_x": proj_x, "proj_z": proj_z, "proj_bc": proj_bc, "proj_dt": proj_dt, "conv_x": conv_x, "conv_bc": conv_bc, "dt_bias": dt_bias, "log_rate": log_rate, "norm_gain": norm_gain, "proj_out": proj_out}


norm_epsilon = 1e-05
highest = lax.Precision.HIGHEST

def causal_conv(values, kernel):
    out_rows = values.shape[0] - kernel.shape[0] + 1
    acc_sum = jnp.zeros((out_rows,) + values.shape[1:], jnp.float32)
    for offset in range(kernel.shape[0]):
        acc_sum = acc_sum + kernel[offset] * values[offset:offset + out_rows]
    return jax.nn.silu(acc_sum).astype(jnp.bfloat16)

def band_mix(head_inner, input_b, read_c, step_dt, log_step, state_in):
    length = head_inner.shape[0]
    cumulative = jnp.cumsum(log_step, axis=0)
    causal = jnp.arange(length)[:, None] >= jnp.arange(length)[None, :]
    decay_gap = cumulative[:, None] - cumulative[None, :]
    decay = jnp.exp(jnp.where(causal[:, :, None, None], decay_gap, -jnp.inf))
    scores = jnp.einsum('tcn,scn->tsc', read_c, input_b, precision=highest)
    weights = decay * scores[:, :, :, None] * step_dt[None]
    diag_out = jnp.einsum('tsch,schp->tchp', weights, head_inner, precision=highest)
    state_out = jnp.einsum('tcn,chnp->tchp', read_c, state_in, precision=highest) * jnp.exp(cumulative)[..., None]
    end_weight = jnp.exp(cumulative[-1][None] - cumulative) * step_dt
    end_state = jnp.einsum('sch,scn,schp->chnp', end_weight, input_b, head_inner, precision=highest)
    return (diag_out + state_out, end_state, cumulative[-1])

def reference(fields, proj_x, proj_z, proj_bc, proj_dt, conv_x, conv_bc, dt_bias, log_rate, norm_gain, proj_out):
    lat_count, lon_count, model_width = fields.shape
    flat_rows = fields.reshape(lat_count * lon_count, model_width)

    def project(weight):
        return jnp.dot(flat_rows, weight, preferred_element_type=jnp.float32).astype(jnp.bfloat16).reshape(lat_count, lon_count, -1)
    inner_pre = project(proj_x)
    gate_pre = project(proj_z)
    bc_pre = project(proj_bc)
    dt_pre = project(proj_dt)
    margin = KERNEL - 1

    def extend(values):
        return jnp.concatenate([jnp.zeros((margin,) + values.shape[1:], jnp.float32), values.astype(jnp.float32)], 0)
    inner_act = causal_conv(extend(inner_pre), conv_x)
    bc_act = causal_conv(extend(bc_pre), conv_bc)
    step_dt = jax.nn.softplus(dt_pre.astype(jnp.float32) + dt_bias)
    log_step = -jnp.exp(log_rate) * step_dt
    head_count = log_rate.shape[0]
    blocks = lat_count // LAT_DEV

    def block_view(values):
        return values.reshape((blocks, LAT_DEV) + values.shape[1:])
    head_inner = inner_act.astype(jnp.float32).reshape(lat_count, lon_count, head_count, HEAD_DIM)
    inputs = (block_view(head_inner), block_view(bc_act[..., :STATE].astype(jnp.float32)), block_view(bc_act[..., STATE:].astype(jnp.float32)), block_view(step_dt), block_view(log_step))

    def advance(carried, pieces):
        band_out, end_state, band_total = band_mix(pieces[0], pieces[1], pieces[2], pieces[3], pieces[4], carried)
        return (jnp.exp(band_total)[..., None, None] * carried + end_state, band_out)
    start_state = jnp.zeros((lon_count, head_count, STATE, HEAD_DIM), jnp.float32)
    final_state, band_outs = lax.scan(advance, start_state, inputs)
    mixed_heads = band_outs.reshape(lat_count, lon_count, head_count * HEAD_DIM)
    gated_out = mixed_heads * jax.nn.silu(gate_pre.astype(jnp.float32))
    normed = gated_out * lax.rsqrt(lax.optimization_barrier(jnp.mean(gated_out * gated_out, -1, keepdims=True)) + norm_epsilon) * norm_gain
    hidden = normed.astype(jnp.bfloat16).reshape(lat_count * lon_count, -1)
    result = jnp.dot(hidden, proj_out, preferred_element_type=jnp.float32).astype(jnp.bfloat16)
    return result.reshape(lat_count, lon_count, model_width)
```

```python
import functools

import jax
import jax.numpy as jnp
from jax import lax
from jax.experimental import pallas as pl
from jax.experimental.pallas import tpu as pltpu
from jax.sharding import Mesh
from jax.sharding import PartitionSpec as P


LAT = ("z", "y")
EPS = 1e-05
HIGHEST = lax.Precision.HIGHEST
F32 = jnp.float32
BF16 = jnp.bfloat16
HALO = 16
LANES = 128


def dot(a, b, **kw):
    return jnp.dot(a, b, preferred_element_type=F32, **kw)


def silu(v):
    return v / (1.0 + jnp.exp(-v))


def halves(v):
    high = v.astype(BF16)
    return high, (v - high.astype(F32)).astype(BF16)


def spread(v, heads, width):
    per = width // heads
    pick = (
        lax.broadcasted_iota(jnp.int32, (heads, width), 1) // per
        == lax.broadcasted_iota(jnp.int32, (heads, width), 0)
    ).astype(BF16)
    high, low = halves(v[:, :heads])
    return dot(high, pick) + dot(low, pick)


def chunk(ref, index):
    return ref[:, pl.ds(pl.multiple_of(index * LANES, LANES), LANES)]


def project_kernel(heads, order, f_ref, halo_ref, *refs):
    w_refs = refs[:8]
    (conv_x, conv_bc, bias, rate, x_out, bc_out, dt_out, cum_out, msg_out, pre) = refs[8:]
    rows, width = x_out.shape
    state = bc_out.shape[1] // 2
    src = jnp.concatenate(
        [
            jnp.concatenate([chunk(halo_ref, order[j]), chunk(f_ref, order[j])], 0)
            for j in range(8)
        ],
        1,
    )
    total = pre.shape[1]
    for n in range(0, total, 256):
        w = jnp.concatenate([r[:, n : n + 256] for r in w_refs], 0)
        pre[:, n : n + 256] = dot(src, w).astype(BF16).astype(F32)
    first = HALO - conv_x.shape[0] + 1

    def conv(at, wide, taps):
        acc = taps[0:1, :] * pre[first : first + rows, at : at + wide]
        for k in range(1, conv_x.shape[0]):
            acc = acc + taps[k : k + 1, :] * pre[first + k : first + k + rows, at : at + wide]
        return silu(acc).astype(BF16)

    step = jax.nn.softplus(pre[HALO:, width + LANES :] + bias[...])
    log_step = -jnp.exp(rate[...]) * step
    lower = (
        lax.broadcasted_iota(jnp.int32, (rows, rows), 0)
        >= lax.broadcasted_iota(jnp.int32, (rows, rows), 1)
    ).astype(F32)
    cum = dot(lower, log_step, precision=HIGHEST)
    dt_out[...] = step
    cum_out[...] = cum
    last = cum[rows - 1 : rows, :]
    weight = jnp.exp(last - cum) * step
    bc = conv(width, 2 * state, conv_bc[...])
    bc_out[...] = bc
    spread_w = spread(weight, heads, width)
    b = bc[:, :state]
    for n in range(0, width, 256):
        x = conv(n, 256, conv_x[:, n : n + 256])
        x_out[:, n : n + 256] = x
        xw = (x.astype(F32) * spread_w[:, n : n + 256]).astype(BF16)
        end = lax.dot_general(b, xw, (((0,), (0,)), ((), ())), preferred_element_type=F32)
        msg_out[:, n : n + 256] = end.astype(BF16)
    high, low = halves(jnp.maximum(last, -104.0))
    msg_out[:, width : width + LANES] = jnp.broadcast_to(high, (state, LANES))
    msg_out[:, width + LANES :] = jnp.broadcast_to(low, (state, LANES))


def within_kernel(heads, x_ref, bc_ref, dt_ref, cum_ref, y_out):
    rows, width = x_ref.shape
    state = bc_ref.shape[1] // 2
    b = bc_ref[:, :state]
    c = bc_ref[:, state:]
    scores = lax.dot_general(c, b, (((1,), (1,)), ((), ())), preferred_element_type=F32)
    causal = lax.broadcasted_iota(jnp.int32, (rows, rows), 0) >= lax.broadcasted_iota(
        jnp.int32, (rows, rows), 1
    )
    cum = cum_ref[...]
    cum_t = cum.T
    dt_t = dt_ref[...].T
    left = lax.broadcasted_iota(jnp.int32, (rows, LANES), 1) < LANES // 2
    for pair in range(heads // 2):
        w = []
        for h in (2 * pair, 2 * pair + 1):
            gap = jnp.where(causal, cum[:, h : h + 1] - cum_t[h : h + 1, :], -jnp.inf)
            w.append((jnp.exp(gap) * (scores * dt_t[h : h + 1, :])).astype(BF16))
        xp = x_ref[:, pair * LANES : (pair + 1) * LANES]
        zero = jnp.zeros_like(xp)
        both = jnp.concatenate([jnp.where(left, xp, zero), jnp.where(left, zero, xp)], 0)
        y_out[:, pair * LANES : (pair + 1) * LANES] = dot(jnp.concatenate(w, 1), both)


def bands_kernel(heads, r_ref, e_out):
    bands, width = e_out.shape
    per = width // heads
    decay = r_ref[:, width : width + LANES].astype(F32) + r_ref[:, width + LANES :].astype(F32)
    row = lax.broadcasted_iota(jnp.int32, (bands, bands), 0)
    col = lax.broadcasted_iota(jnp.int32, (bands, bands), 1)
    upto = dot((row >= col).astype(F32), decay, precision=HIGHEST)
    before = upto - decay
    upto_t = upto.T
    left = lax.broadcasted_iota(jnp.int32, (bands, LANES), 1) < per
    for pair in range(heads // 2):
        w = []
        for h in (2 * pair, 2 * pair + 1):
            gap = jnp.where(row > col, before[:, h : h + 1] - upto_t[h : h + 1, :], -jnp.inf)
            w.append(jnp.exp(gap).astype(BF16))
        s = r_ref[:, pair * LANES : (pair + 1) * LANES]
        zero = jnp.zeros_like(s)
        both = jnp.concatenate([jnp.where(left, s, zero), jnp.where(left, zero, s)], 0)
        e_out[:, pair * LANES : (pair + 1) * LANES] = dot(jnp.concatenate(w, 1), both).astype(BF16)


def gate_kernel(order, f_ref, *refs):
    w_refs, out = refs[:8], refs[8]
    src = jnp.concatenate([chunk(f_ref, order[j]) for j in range(8)], 1)
    for n in range(0, out.shape[1], 256):
        w = jnp.concatenate([r[:, n : n + 256] for r in w_refs], 0)
        out[:, n : n + 256] = silu(dot(src, w).astype(BF16).astype(F32))


def finish_kernel(heads, order, y_ref, in_ref, bc_ref, cum_ref, gate_ref, gain, *refs):
    w_refs, out, hidden = refs[:8], refs[8], refs[9]
    rows, width = y_ref.shape
    state = bc_ref.shape[1] // 2
    c = bc_ref[:, state:]
    grown = spread(jnp.exp(cum_ref[...]), heads, width)
    square = jnp.zeros((rows, 1), F32)
    parts = []
    for n in range(0, width, 256):
        y = y_ref[:, n : n + 256] + dot(c, in_ref[:, n : n + 256]) * grown[:, n : n + 256]
        g = y * gate_ref[:, n : n + 256]
        square = square + jnp.sum(g * g, -1, keepdims=True)
        parts.append(g)
    scale = lax.rsqrt(square / width + EPS)
    for i, n in enumerate(range(0, width, 256)):
        hidden[:, n : n + 256] = (parts[i] * scale * gain[:, n : n + 256]).astype(BF16)
    src = jnp.concatenate([chunk(hidden, order[j]) for j in range(8)], 1)
    base = w_refs[0].shape[1] - out.shape[1]
    for n in range(0, out.shape[1], 256):
        w = jnp.concatenate([r[:, base + n : base + n + 256] for r in w_refs], 0)
        out[:, n : n + 256] = dot(src, w).astype(BF16)


def call(body, outs, args, smem=0, scratch=(), flops=0, name=None):
    vmem = pl.BlockSpec(memory_space=pltpu.VMEM)
    specs = [pl.BlockSpec(memory_space=pltpu.SMEM)] * smem + [vmem] * (len(args) - smem)
    nbytes = sum(a.size * a.dtype.itemsize for a in args)
    return pl.pallas_call(
        body,
        out_shape=outs,
        in_specs=specs,
        out_specs=jax.tree.map(lambda _: vmem, outs),
        scratch_shapes=list(scratch),
        cost_estimate=pl.CostEstimate(flops=flops, bytes_accessed=nbytes, transcendentals=0),
        name=name,
    )(*args)


def around(block):
    n = lax.axis_size("x")
    shards = [block]
    for d in range(1, n):
        shards.append(lax.ppermute(block, "x", [(i, (i + d) % n) for i in range(n)]))
    return shards


def other_core(blocks):
    return [lax.ppermute(b, "c", [(0, 1), (1, 0)]) for b in blocks]


def padded(a, width):
    return jnp.pad(a, [(0, 0)] * (a.ndim - 1) + [(0, width - a.shape[-1])])


def local(
    fields, proj_x, proj_z, proj_bc, proj_dt, conv_x, conv_bc, dt_bias, log_rate, norm_gain, proj_out
):
    rows, _, depth = fields.shape
    heads = log_rate.shape[0]
    width = proj_x.shape[1]
    state = proj_bc.shape[1] // 2
    n_x = lax.axis_size("x")
    bands = lax.axis_size(LAT)
    f = fields.reshape(rows, depth)
    halo = lax.ppermute(f[rows - HALO :], LAT, [(i, i + 1) for i in range(bands - 1)])
    first = jnp.concatenate([proj_x, proj_bc, padded(proj_dt, LANES)], 1)
    mine = around(first)
    x_at, c_at = lax.axis_index("x"), lax.axis_index("c")
    x_of = (x_at - jnp.arange(n_x) + n_x) % n_x
    order = jnp.concatenate([x_of * 2 + c_at, x_of * 2 + 1 - c_at]).astype(jnp.int32)
    w1 = mine + other_core(mine)
    second = jnp.concatenate([proj_z, proj_out], 1)
    second, _ = lax.optimization_barrier((second, mine))
    mine2 = around(second)
    w2 = mine2 + other_core(mine2)

    sds = jax.ShapeDtypeStruct
    x_act, bc_act, step, cum, msg = call(
        functools.partial(project_kernel, heads),
        (
            sds((rows, width), BF16),
            sds((rows, 2 * state), BF16),
            sds((rows, LANES), F32),
            sds((rows, LANES), F32),
            sds((state, width + 2 * LANES), BF16),
        ),
        [order, f, halo, *w1, conv_x, conv_bc]
        + [padded(dt_bias[None], LANES), padded(log_rate[None], LANES)],
        smem=1,
        scratch=[pltpu.VMEM((HALO + rows, first.shape[1]), F32)],
        flops=2 * rows * depth * first.shape[1],
        name="project",
    )
    assert state == bands
    got = lax.all_to_all(msg, LAT, 0, 0, tiled=True)
    y = call(
        functools.partial(within_kernel, heads),
        sds((rows, width), F32),
        [x_act, bc_act, step, cum],
        flops=2 * rows * rows * width * 2,
        name="within",
    )
    entering = call(
        functools.partial(bands_kernel, heads),
        sds((bands, width), BF16),
        [got],
        flops=2 * bands * bands * width,
        name="bands",
    )
    incoming = lax.all_to_all(entering, LAT, 0, 0, tiled=True)
    gate = call(
        gate_kernel,
        sds((rows, width), F32),
        [order, f, *w2],
        smem=1,
        flops=2 * rows * depth * width,
        name="gate",
    )
    out = call(
        functools.partial(finish_kernel, heads),
        sds((rows, depth), BF16),
        [order, y, incoming, bc_act, cum, gate, norm_gain[None], *w2],
        smem=1,
        scratch=[pltpu.VMEM((rows, width), BF16)],
        flops=2 * rows * depth * width,
        name="finish",
    )
    return out.reshape(rows, 1, depth)


def solution(mesh):
    finer = Mesh(mesh.devices.reshape(8, 8, 4, 2), ("z", "y", "x", "c"))
    lat, lon = P(LAT, ("x", "c"), None), P(("x", "c"), None)
    return jax.shard_map(
        local,
        mesh=finer,
        in_specs=(lat, lon, lon, lon, lon, P(), P(), P(), P(), P(), lon),
        out_specs=lat,
        check_vma=False,
    )
```

```python
import jax
import jax.numpy as jnp
from jax import lax
from jax.experimental import pallas as pl
from jax.experimental.pallas import tpu as pltpu
from jax.sharding import Mesh
from jax.sharding import PartitionSpec as P


LAT = ("z", "y")
EPS = 1e-05
HIGHEST = lax.Precision.HIGHEST
F32 = jnp.float32
BF16 = jnp.bfloat16
HALO = 16
LANES = 128
SUB = 8
TILE = 256


def dot(a, b, **kw):
    return jnp.dot(a, b, preferred_element_type=F32, **kw)


def dot_nt(a, b):
    return lax.dot_general(a, b, (((1,), (1,)), ((), ())), preferred_element_type=F32)


def dot_tn(a, b):
    return lax.dot_general(a, b, (((0,), (0,)), ((), ())), preferred_element_type=F32)


def iota(shape, dim):
    return lax.broadcasted_iota(jnp.int32, shape, dim)


def silu(v):
    return v / (1.0 + jnp.exp(-v))


def halves(v):
    high = v.astype(BF16)
    return high, (v - high.astype(F32)).astype(BF16)


def spread(v, width):
    heads = v.shape[1]
    shape = (heads, width)
    pick = (iota(shape, 1) // (width // heads) == iota(shape, 0)).astype(BF16)
    high, low = halves(v)
    return dot(high, pick) + dot(low, pick)


def chunk(ref, index):
    return ref[:, pl.ds(pl.multiple_of(index * LANES, LANES), LANES)]


def ordered(ref, order, n):
    return jnp.concatenate([chunk(ref, order[j]) for j in range(n)], 1)


def stacked(refs, rows, columns):
    return jnp.concatenate([r[rows, columns] for r in refs], 0)


def pack_kernel(x_ref, bc_ref, dt_ref, out):
    k = x_ref.shape[0]
    blocks = x_ref.shape[1] // LANES
    part = k // blocks
    bc = jnp.concatenate([bc_ref[j * part : (j + 1) * part, :] for j in range(blocks)], 1)
    for i in range(out.shape[0]):
        out[i, :k, :] = x_ref[...]
        out[i, k : k + part, :] = bc
        out[i, k + part :, :LANES] = dt_ref[...]
        out[i, k + part :, LANES:] = jnp.zeros((part, x_ref.shape[1] - LANES), BF16)


def project_kernel(
    order, f_ref, halo_ref, wa, wb, conv_x, conv_bc, bias, rate,
    x_out, bc_out, dt_out, cum_out, msg_out, pre,
):
    rows, width = x_out.shape
    heads = bias.shape[1]
    half = width // 2
    k = LANES
    n = 2 * wa.shape[0]
    blocks = width // LANES
    part = k // blocks
    shards = [r.at[i] for r in (wa, wb) for i in range(n // 2)]
    src = jnp.concatenate([ordered(halo_ref, order, n), ordered(f_ref, order, n)], 0)
    first = HALO - conv_x.shape[0] + 1

    def conv(at, wide, taps):
        acc = taps[0:1, :] * pre[first : first + rows, at : at + wide]
        for i in range(1, conv_x.shape[0]):
            acc = acc + taps[i : i + 1, :] * pre[first + i : first + i + rows, at : at + wide]
        return silu(acc)

    w_dt = jnp.concatenate([r[i, k + part :, :LANES] for r in (wa, wb) for i in range(n // 2)], 1)
    dt_pre = dot_nt(src[HALO:], w_dt).astype(BF16).astype(F32)
    step = jax.nn.softplus(dt_pre + bias[...])
    log_step = -jnp.exp(rate[...]) * step
    lower = (iota((rows, rows), 0) >= iota((rows, rows), 1)).astype(F32)
    cum = dot(lower, log_step, precision=HIGHEST)
    dt_out[...] = step
    cum_out[...] = cum
    last = cum[rows - 1 : rows, :]
    weight = spread(jnp.exp(last - cum) * step, width)

    w_bc = jnp.concatenate(
        [
            r[i, k : k + part, j * LANES : (j + 1) * LANES]
            for r in (wa, wb)
            for i in range(n // 2)
            for j in range(blocks)
        ],
        0,
    )
    pre[:, width:] = dot(src, w_bc).astype(BF16).astype(F32)
    bc = conv(width, LANES, conv_bc[...])
    bc_out[...] = bc.astype(BF16)
    left = iota((rows, LANES), 1) < LANES // 2
    b0 = jnp.where(left, bc, 0.0)
    b = (b0.astype(BF16), pltpu.roll(b0, LANES // 2, 1).astype(BF16))

    def end(at, q):
        pre[:, at : at + TILE] = (
            dot(src, stacked(shards, slice(0, k), slice(at, at + TILE))).astype(BF16).astype(F32)
        )
        x = conv(at, TILE, conv_x[:, at : at + TILE]).astype(BF16)
        x_out[:, at : at + TILE] = x
        xw = (x.astype(F32) * weight[:, at : at + TILE]).astype(BF16)
        return dot_tn(xw, b[q])

    for at in range(0, half, TILE):
        t = end(at, 0) + end(half + at, 1)
        msg_out[at // SUB : (at + TILE) // SUB, :SUB, :] = t.reshape(TILE // SUB, SUB, LANES).astype(BF16)
    pairs = heads // 2
    mine = iota((pairs, heads), 1) % pairs == iota((pairs, heads), 0)
    pick = (iota((heads, LANES), 1) // (LANES // 2) == iota((heads, LANES), 0) // pairs).astype(BF16)
    high, low = (dot(jnp.where(mine, v.astype(F32), 0.0).astype(BF16), pick) for v in halves(last))
    row = iota((SUB, LANES), 0)
    each = msg_out.shape[0] // pairs
    for j in range(pairs):
        tail = jnp.where(row == 0, high[j : j + 1, :], jnp.where(row == 1, low[j : j + 1, :], 0.0))
        for i in range(each):
            msg_out[j * each + i, SUB:, :] = tail.astype(BF16)


def within_kernel(x_ref, bc_ref, dt_ref, cum_ref, y_out):
    rows, _ = x_ref.shape
    heads = dt_ref.shape[1]
    state = bc_ref.shape[1] // 2
    scores = dot_nt(bc_ref[:, state:], bc_ref[:, :state])
    causal = iota((rows, rows), 0) >= iota((rows, rows), 1)
    cum = cum_ref[...]
    cum_t = cum.T
    dt_t = dt_ref[...].T
    left = iota((rows, LANES), 1) < LANES // 2
    for pair in range(heads // 2):
        w = []
        for h in (2 * pair, 2 * pair + 1):
            gap = jnp.where(causal, cum[:, h : h + 1] - cum_t[h : h + 1, :], -jnp.inf)
            w.append((jnp.exp(gap) * (scores * dt_t[h : h + 1, :])).astype(BF16))
        xp = x_ref[:, pair * LANES : (pair + 1) * LANES]
        zero = jnp.zeros_like(xp)
        both = jnp.concatenate([jnp.where(left, xp, zero), jnp.where(left, zero, xp)], 0)
        y_out[:, pair * LANES : (pair + 1) * LANES] = dot(jnp.concatenate(w, 1), both)


def bands_kernel(r_ref, e_out):
    carry = jnp.zeros(e_out.shape[1:], F32)
    for b in range(e_out.shape[0]):
        e_out[b] = carry.astype(BF16)
        tail = r_ref[b, SUB:, :].astype(F32)
        carry = jnp.exp(tail[0:1, :] + tail[1:2, :]) * carry + r_ref[b, :SUB, :].astype(F32)


def gate_kernel(order, f_ref, *refs):
    shards, out = refs[:-1], refs[-1]
    src = ordered(f_ref, order, len(shards))
    for at in range(0, out.shape[1], TILE):
        w = stacked(shards, slice(0, LANES), slice(at, at + TILE))
        out[:, at : at + TILE] = silu(dot(src, w).astype(BF16).astype(F32))


def finish_kernel(order, y_ref, in_ref, bc_ref, cum_ref, gate_ref, gain, *refs):
    shards, (out, hidden) = refs[:-2], refs[-2:]
    rows, width = y_ref.shape
    half = width // 2
    bc = bc_ref[...].astype(F32)
    left = iota((rows, LANES), 1) < LANES // 2
    c1 = jnp.where(left, 0.0, bc)
    c = (pltpu.roll(c1, LANES // 2, 1).astype(BF16), c1.astype(BF16))
    grown = spread(jnp.exp(cum_ref[...]), width)
    square = jnp.zeros((rows, 1), F32)
    parts = []
    for at in range(0, width, TILE):
        inner = in_ref[at % half : at % half + TILE, :]
        y = y_ref[:, at : at + TILE] + dot_nt(c[at // half], inner) * grown[:, at : at + TILE]
        g = y * gate_ref[:, at : at + TILE]
        square = square + jnp.sum(g * g, -1, keepdims=True)
        parts.append(g)
    scale = lax.rsqrt(square / width + EPS)
    for i, at in enumerate(range(0, width, TILE)):
        hidden[:, at : at + TILE] = (parts[i] * scale * gain[:, at : at + TILE]).astype(BF16)
    src = ordered(hidden, order, len(shards))
    for at in range(0, out.shape[1], TILE):
        w = stacked(shards, slice(LANES, 2 * LANES), slice(at, at + TILE))
        out[:, at : at + TILE] = dot(src, w).astype(BF16)


def call(body, outs, args, smem=0, scratch=(), flops=0):
    vmem = pl.BlockSpec(memory_space=pltpu.VMEM)
    specs = [pl.BlockSpec(memory_space=pltpu.SMEM)] * smem + [vmem] * (len(args) - smem)
    nbytes = sum(a.size * a.dtype.itemsize for a in args)
    return pl.pallas_call(
        body,
        out_shape=outs,
        in_specs=specs,
        out_specs=jax.tree.map(lambda _: vmem, outs),
        scratch_shapes=list(scratch),
        compiler_params=pltpu.CompilerParams(vmem_limit_bytes=24 * 2**20),
        cost_estimate=pl.CostEstimate(flops=flops, bytes_accessed=nbytes, transcendentals=0),
    )(*args)


def other_core(block):
    return lax.ppermute(block, "c", [(0, 1), (1, 0)])


def local(
    fields, proj_x, proj_z, proj_bc, proj_dt, conv_x, conv_bc, dt_bias, log_rate, norm_gain, proj_out
):
    rows, _, depth = fields.shape
    heads = log_rate.shape[0]
    width = proj_x.shape[1]
    state = proj_bc.shape[1] // 2
    n_x = lax.axis_size("x")
    bands = lax.axis_size(LAT)
    f = fields.reshape(rows, depth)
    sds = jax.ShapeDtypeStruct

    k = proj_x.shape[0]
    first = call(
        pack_kernel,
        sds((n_x, k + 2 * k * LANES // width, width), BF16),
        [proj_x, proj_bc, proj_dt.T],
    )
    w1a = lax.all_to_all(first, "x", 0, 0)
    halo = lax.ppermute(f[rows - HALO :], LAT, [(i, i + 1) for i in range(bands - 1)])
    x_at, c_at = lax.axis_index("x"), lax.axis_index("c")
    x_all = jnp.arange(n_x)
    order = jnp.concatenate([x_all * 2 + c_at, x_all * 2 + 1 - c_at]).astype(jnp.int32)
    x_near = (x_at - x_all + n_x) % n_x
    order2 = jnp.concatenate([x_near * 2 + c_at, x_near * 2 + 1 - c_at]).astype(jnp.int32)
    second = jnp.concatenate([proj_z, proj_out], 0)
    w1a, halo, second, order, order2 = lax.optimization_barrier((w1a, halo, second, order, order2))
    w1b = other_core(w1a)
    w2a, w2b = [second], []
    for d in range(1, n_x):
        w2a.append(lax.ppermute(second, "x", [(i, (i + d) % n_x) for i in range(n_x)]))
    for d in range(n_x):
        w2b.append(other_core(w2a[d]))

    x_act, bc_act, step, cum, msg = call(
        project_kernel,
        (
            sds((rows, width), BF16),
            sds((rows, 2 * state), BF16),
            sds((rows, heads), F32),
            sds((rows, heads), F32),
            sds((bands, 2 * SUB, LANES), BF16),
        ),
        [order, f, halo, w1a, w1b, conv_x, conv_bc, dt_bias[None], log_rate[None]],
        smem=1,
        scratch=[pltpu.VMEM((HALO + rows, width + 2 * state), F32)],
        flops=2 * rows * depth * (width + 2 * LANES),
    )
    got = lax.all_to_all(msg, LAT, 0, 0)
    y = call(
        within_kernel,
        sds((rows, width), F32),
        [x_act, bc_act, step, cum],
        flops=2 * rows * rows * width * 2,
    )
    entering = call(
        bands_kernel, sds((bands, SUB, LANES), BF16), [got], flops=bands * SUB * LANES * 100
    )
    incoming = lax.all_to_all(entering, LAT, 0, 0)
    incoming = incoming.reshape(bands * SUB, LANES)
    gate = call(
        gate_kernel,
        sds((rows, width), F32),
        [order2, f, *w2a, *w2b],
        smem=1,
        flops=2 * rows * depth * width,
    )
    out = call(
        finish_kernel,
        sds((rows, depth), BF16),
        [order2, y, incoming, bc_act, cum, gate, norm_gain[None], *w2a, *w2b],
        smem=1,
        scratch=[pltpu.VMEM((rows, width), BF16)],
        flops=2 * rows * depth * width,
    )
    return out.reshape(rows, 1, depth)


def solution(mesh):
    finer = Mesh(mesh.devices.reshape(8, 8, 4, 2), ("z", "y", "x", "c"))
    lat, lon = P(LAT, ("x", "c"), None), P(("x", "c"), None)
    return jax.shard_map(
        local,
        mesh=finer,
        in_specs=(lat, lon, lon, lon, lon, P(), P(), P(), P(), P(), lon),
        out_specs=lat,
        check_vma=False,
    )
```

```python
import jax
import jax.numpy as jnp
from jax import lax
from jax.experimental import pallas as pl
from jax.experimental.pallas import tpu as pltpu
from jax.sharding import Mesh
from jax.sharding import PartitionSpec as P


LAT = ("z", "y")
EPS = 1e-05
HIGHEST = lax.Precision.HIGHEST
F32 = jnp.float32
BF16 = jnp.bfloat16
HALO = 16
LANES = 128
SUB = 8
TILE = 256


def dot(a, b, **kw):
    return jnp.dot(a, b, preferred_element_type=F32, **kw)


def dot_nt(a, b):
    return lax.dot_general(a, b, (((1,), (1,)), ((), ())), preferred_element_type=F32)


def dot_tn(a, b):
    return lax.dot_general(a, b, (((0,), (0,)), ((), ())), preferred_element_type=F32)


def iota(shape, dim):
    return lax.broadcasted_iota(jnp.int32, shape, dim)


def silu(v):
    return v / (1.0 + jnp.exp(-v))


def halves(v):
    high = v.astype(BF16)
    return high, (v - high.astype(F32)).astype(BF16)


def spread(v, width):
    heads = v.shape[1]
    shape = (heads, width)
    pick = (iota(shape, 1) // (width // heads) == iota(shape, 0)).astype(BF16)
    high, low = halves(v)
    return dot(high, pick) + dot(low, pick)


def chunk(ref, index):
    return ref[:, pl.ds(pl.multiple_of(index * LANES, LANES), LANES)]


def ordered(ref, order, n):
    return jnp.concatenate([chunk(ref, order[j]) for j in range(n)], 1)


def stacked(refs, rows, columns):
    return jnp.concatenate([r[rows, columns] for r in refs], 0)


def fetch(pairs, sems):
    copies = [pltpu.make_async_copy(a, b, sems.at[i]) for i, (a, b) in enumerate(pairs)]
    for c in copies:
        c.start()
    return copies


def pack_kernel(x_ref, bc_ref, dt_ref, out, x, bc, dt, sems):
    copies = fetch([(x_ref, x), (bc_ref, bc), (dt_ref, dt)], sems)
    k, width = x.shape
    blocks = width // LANES
    part = k // blocks
    for c in copies:
        c.wait()
    rest = jnp.zeros((part, width - LANES), BF16)
    for i in range(out.shape[0]):
        out[i, :k, :] = x[...]
        for j in range(blocks):
            out[i, k : k + part, j * LANES : (j + 1) * LANES] = bc[j * part : (j + 1) * part, :]
        out[i, k + part :, :LANES] = dt[...]
        out[i, k + part :, LANES:] = rest


def source_kernel(order, f_ref, halo_ref, out):
    n = out.shape[1] // LANES
    for j in range(n):
        at = slice(j * LANES, (j + 1) * LANES)
        out[:HALO, at] = chunk(halo_ref, order[j])
        out[HALO:, at] = chunk(f_ref, order[j])


def project_kernel(
    src_ref, wa, wb, conv_x, conv_bc, bias, rate,
    x_out, bc_out, dt_out, cum_out, msg_out, pre,
):
    rows, width = x_out.shape
    heads = bias.shape[1]
    half = width // 2
    k = LANES
    n = 2 * wa.shape[0]
    blocks = width // LANES
    part = k // blocks
    shards = [r.at[i] for r in (wa, wb) for i in range(n // 2)]
    src = src_ref[...]
    first = HALO - conv_x.shape[0] + 1

    def conv(at, wide, taps):
        acc = taps[0:1, :] * pre[first : first + rows, at : at + wide]
        for i in range(1, conv_x.shape[0]):
            acc = acc + taps[i : i + 1, :] * pre[first + i : first + i + rows, at : at + wide]
        return silu(acc)

    w_dt = jnp.concatenate([r[i, k + part :, :LANES] for r in (wa, wb) for i in range(n // 2)], 1)
    dt_pre = dot_nt(src[HALO:], w_dt).astype(BF16).astype(F32)
    step = jax.nn.softplus(dt_pre + bias[...])
    log_step = -jnp.exp(rate[...]) * step
    lower = (iota((rows, rows), 0) >= iota((rows, rows), 1)).astype(F32)
    cum = dot(lower, log_step, precision=HIGHEST)
    dt_out[...] = step
    cum_out[...] = cum
    last = cum[rows - 1 : rows, :]
    weight = spread(jnp.exp(last - cum) * step, width)

    w_bc = jnp.concatenate(
        [
            r[i, k : k + part, j * LANES : (j + 1) * LANES]
            for r in (wa, wb)
            for i in range(n // 2)
            for j in range(blocks)
        ],
        0,
    )
    pre[:, width:] = dot(src, w_bc).astype(BF16).astype(F32)
    bc = conv(width, LANES, conv_bc[...])
    bc_out[...] = bc.astype(BF16)
    left = iota((rows, LANES), 1) < LANES // 2
    b0 = jnp.where(left, bc, 0.0)
    b = (b0.astype(BF16), pltpu.roll(b0, LANES // 2, 1).astype(BF16))

    def end(at, q):
        pre[:, at : at + TILE] = (
            dot(src, stacked(shards, slice(0, k), slice(at, at + TILE))).astype(BF16).astype(F32)
        )
        x = conv(at, TILE, conv_x[:, at : at + TILE]).astype(BF16)
        x_out[:, at : at + TILE] = x
        xw = (x.astype(F32) * weight[:, at : at + TILE]).astype(BF16)
        return dot_tn(xw, b[q])

    for at in range(0, half, TILE):
        t = end(at, 0) + end(half + at, 1)
        msg_out[at // SUB : (at + TILE) // SUB, :SUB, :] = t.reshape(TILE // SUB, SUB, LANES).astype(BF16)
    pairs = heads // 2
    mine = iota((pairs, heads), 1) % pairs == iota((pairs, heads), 0)
    pick = (iota((heads, LANES), 1) // (LANES // 2) == iota((heads, LANES), 0) // pairs).astype(BF16)
    high, low = (dot(jnp.where(mine, v.astype(F32), 0.0).astype(BF16), pick) for v in halves(last))
    row = iota((SUB, LANES), 0)
    each = msg_out.shape[0] // pairs
    for j in range(pairs):
        tail = jnp.where(row == 0, high[j : j + 1, :], jnp.where(row == 1, low[j : j + 1, :], 0.0))
        for i in range(each):
            msg_out[j * each + i, SUB:, :] = tail.astype(BF16)


def within_kernel(x_ref, bc_ref, dt_ref, cum_ref, y_out):
    rows, _ = x_ref.shape
    heads = dt_ref.shape[1]
    state = bc_ref.shape[1] // 2
    scores = dot_nt(bc_ref[:, state:], bc_ref[:, :state])
    causal = iota((rows, rows), 0) >= iota((rows, rows), 1)
    cum = cum_ref[...]
    cum_t = cum.T
    dt_t = dt_ref[...].T
    left = iota((rows, LANES), 1) < LANES // 2
    for pair in range(heads // 2):
        w = []
        for h in (2 * pair, 2 * pair + 1):
            gap = jnp.where(causal, cum[:, h : h + 1] - cum_t[h : h + 1, :], -jnp.inf)
            w.append((jnp.exp(gap) * (scores * dt_t[h : h + 1, :])).astype(BF16))
        xp = x_ref[:, pair * LANES : (pair + 1) * LANES]
        zero = jnp.zeros_like(xp)
        both = jnp.concatenate([jnp.where(left, xp, zero), jnp.where(left, zero, xp)], 0)
        y_out[:, pair * LANES : (pair + 1) * LANES] = dot(jnp.concatenate(w, 1), both)


def bands_kernel(r_ref, e_out):
    carry = jnp.zeros(e_out.shape[1:], F32)
    for b in range(e_out.shape[0]):
        e_out[b] = carry.astype(BF16)
        tail = r_ref[b, SUB:, :].astype(F32)
        carry = jnp.exp(tail[0:1, :] + tail[1:2, :]) * carry + r_ref[b, :SUB, :].astype(F32)


def gate_kernel(order, f_ref, *refs):
    shards, (out, w, sems) = refs[:-3], refs[-3:]
    k = w.shape[0] // len(shards)
    copies = fetch([(r.at[:k], w.at[pl.ds(i * k, k)]) for i, r in enumerate(shards)], sems)
    src = ordered(f_ref, order, len(shards))
    for c in copies:
        c.wait()
    for at in range(0, out.shape[1], TILE):
        out[:, at : at + TILE] = dot(src, w[:, at : at + TILE]).astype(BF16)


def finish_kernel(order, y_ref, in_ref, bc_ref, cum_ref, gate_ref, gain, *refs):
    shards, (out, hidden, w, sems) = refs[:-4], refs[-4:]
    k = w.shape[0] // len(shards)
    copies = fetch([(r.at[k:], w.at[pl.ds(i * k, k)]) for i, r in enumerate(shards)], sems)
    rows, width = y_ref.shape
    half = width // 2
    bc = bc_ref[...].astype(F32)
    left = iota((rows, LANES), 1) < LANES // 2
    c1 = jnp.where(left, 0.0, bc)
    c = (pltpu.roll(c1, LANES // 2, 1).astype(BF16), c1.astype(BF16))
    grown = spread(jnp.exp(cum_ref[...]), width)
    square = jnp.zeros((rows, 1), F32)
    parts = []
    for at in range(0, width, TILE):
        inner = in_ref[at % half : at % half + TILE, :]
        y = y_ref[:, at : at + TILE] + dot_nt(c[at // half], inner) * grown[:, at : at + TILE]
        g = y * silu(gate_ref[:, at : at + TILE].astype(F32))
        square = square + jnp.sum(g * g, -1, keepdims=True)
        parts.append(g)
    scale = lax.rsqrt(square / width + EPS)
    for i, at in enumerate(range(0, width, TILE)):
        hidden[:, at : at + TILE] = (parts[i] * scale * gain[:, at : at + TILE]).astype(BF16)
    src = ordered(hidden, order, len(shards))
    for c in copies:
        c.wait()
    for at in range(0, out.shape[1], TILE):
        out[:, at : at + TILE] = dot(src, w[:, at : at + TILE]).astype(BF16)


def call(body, outs, args, smem=0, hbm=0, scratch=(), flops=0):
    vmem = pl.BlockSpec(memory_space=pltpu.VMEM)
    specs = (
        [pl.BlockSpec(memory_space=pltpu.SMEM)] * smem
        + [vmem] * (len(args) - smem - hbm)
        + [pl.BlockSpec(memory_space=pltpu.MemorySpace.HBM)] * hbm
    )
    args = [
        pltpu.with_memory_space_constraint(a, pltpu.MemorySpace.HBM) if i >= len(args) - hbm else a
        for i, a in enumerate(args)
    ]
    scratch = list(scratch) + ([pltpu.SemaphoreType.DMA((hbm,))] if hbm else [])
    nbytes = sum(a.size * a.dtype.itemsize for a in args)
    return pl.pallas_call(
        body,
        out_shape=outs,
        in_specs=specs,
        out_specs=jax.tree.map(lambda _: vmem, outs),
        scratch_shapes=scratch,
        compiler_params=pltpu.CompilerParams(vmem_limit_bytes=16 * 2**20),
        cost_estimate=pl.CostEstimate(flops=flops, bytes_accessed=nbytes, transcendentals=0),
    )(*args)


def other_core(block):
    return lax.ppermute(block, "c", [(0, 1), (1, 0)])


def local(
    fields, proj_x, proj_z, proj_bc, proj_dt, conv_x, conv_bc, dt_bias, log_rate, norm_gain, proj_out
):
    rows, _, depth = fields.shape
    heads = log_rate.shape[0]
    width = proj_x.shape[1]
    state = proj_bc.shape[1] // 2
    n_x = lax.axis_size("x")
    bands = lax.axis_size(LAT)
    f = fields.reshape(rows, depth)
    sds = jax.ShapeDtypeStruct

    k = proj_x.shape[0]
    first = call(
        pack_kernel,
        sds((n_x, k + 2 * k * LANES // width, width), BF16),
        [proj_x, proj_bc, proj_dt.T],
        hbm=3,
        scratch=[
            pltpu.VMEM(proj_x.shape, BF16),
            pltpu.VMEM(proj_bc.shape, BF16),
            pltpu.VMEM(proj_dt.shape[::-1], BF16),
        ],
    )
    w1a = lax.all_to_all(first, "x", 0, 0)
    halo = lax.ppermute(f[rows - HALO :], LAT, [(i, i + 1) for i in range(bands - 1)])
    x_at, c_at = lax.axis_index("x"), lax.axis_index("c")
    x_all = jnp.arange(n_x)
    order = jnp.concatenate([x_all * 2 + c_at, x_all * 2 + 1 - c_at]).astype(jnp.int32)
    x_near = (x_at - x_all + n_x) % n_x
    order2 = jnp.concatenate([x_near * 2 + c_at, x_near * 2 + 1 - c_at]).astype(jnp.int32)
    second = jnp.concatenate([proj_z, proj_out], 0)
    src = call(
        source_kernel, sds((HALO + rows, depth), BF16), [order, f, halo], smem=1, flops=10**6
    )
    w2a, w2b = [second], []
    for d in range(1, n_x):
        w2a.append(lax.ppermute(second, "x", [(i, (i + d) % n_x) for i in range(n_x)]))
    w1a, src, order2 = lax.optimization_barrier((w1a, src, order2))
    w1b = other_core(w1a)
    for d in range(n_x):
        w2b.append(other_core(w2a[d]))

    x_act, bc_act, step, cum, msg = call(
        project_kernel,
        (
            sds((rows, width), BF16),
            sds((rows, 2 * state), BF16),
            sds((rows, heads), F32),
            sds((rows, heads), F32),
            sds((bands, 2 * SUB, LANES), BF16),
        ),
        [src, w1a, w1b, conv_x, conv_bc, dt_bias[None], log_rate[None]],
        scratch=[pltpu.VMEM((HALO + rows, width + 2 * state), F32)],
        flops=2 * rows * depth * (width + 2 * LANES),
    )
    got = lax.all_to_all(msg, LAT, 0, 0)
    y = call(
        within_kernel,
        sds((rows, width), F32),
        [x_act, bc_act, step, cum],
        flops=2 * rows * rows * width * 2,
    )
    entering = call(
        bands_kernel, sds((bands, SUB, LANES), BF16), [got], flops=bands * SUB * LANES * 100
    )
    incoming = lax.all_to_all(entering, LAT, 0, 0)
    incoming = incoming.reshape(bands * SUB, LANES)
    gate = call(
        gate_kernel,
        sds((rows, width), BF16),
        [order2, f, *w2a, *w2b],
        smem=1,
        hbm=2 * n_x,
        scratch=[pltpu.VMEM((depth, width), BF16)],
        flops=2 * rows * depth * width,
    )
    out = call(
        finish_kernel,
        sds((rows, depth), BF16),
        [order2, y, incoming, bc_act, cum, gate, norm_gain[None], *w2a, *w2b],
        smem=1,
        hbm=2 * n_x,
        scratch=[pltpu.VMEM((rows, width), BF16), pltpu.VMEM((width, depth), BF16)],
        flops=2 * rows * depth * width,
    )
    return out.reshape(rows, 1, depth)


def solution(mesh):
    finer = Mesh(mesh.devices.reshape(8, 8, 4, 2), ("z", "y", "x", "c"))
    lat, lon = P(LAT, ("x", "c"), None), P(("x", "c"), None)
    return jax.shard_map(
        local,
        mesh=finer,
        in_specs=(lat, lon, lon, lon, lon, P(), P(), P(), P(), P(), lon),
        out_specs=lat,
        check_vma=False,
    )
```

```python
import functools

import jax
import jax.numpy as jnp
from jax import lax
from jax.experimental import pallas as pl
from jax.experimental.pallas import tpu as pltpu
from jax.sharding import Mesh
from jax.sharding import PartitionSpec as P


LAT = ("z", "y")
EPS = 1e-05
HIGHEST = lax.Precision.HIGHEST
F32 = jnp.float32
BF16 = jnp.bfloat16
HALO = 16
LANES = 128
SUB = 8
TILE = 256


def dot(a, b, **kw):
    return jnp.dot(a, b, preferred_element_type=F32, **kw)


def dot_nt(a, b):
    return lax.dot_general(a, b, (((1,), (1,)), ((), ())), preferred_element_type=F32)


def dot_tn(a, b):
    return lax.dot_general(a, b, (((0,), (0,)), ((), ())), preferred_element_type=F32)


def iota(shape, dim):
    return lax.broadcasted_iota(jnp.int32, shape, dim)


def silu(v):
    return v / (1.0 + jnp.exp(-v))


def halves(v):
    high = v.astype(BF16)
    return high, (v - high.astype(F32)).astype(BF16)


def spread(v, width):
    heads = v.shape[1]
    shape = (heads, width)
    pick = (iota(shape, 1) // (width // heads) == iota(shape, 0)).astype(BF16)
    high, low = halves(v)
    return dot(high, pick) + dot(low, pick)


def chunk(ref, index):
    return ref[:, pl.ds(pl.multiple_of(index * LANES, LANES), LANES)]


def ordered(ref, order, n):
    return jnp.concatenate([chunk(ref, order[j]) for j in range(n)], 1)


def stacked(refs, rows, columns):
    return jnp.concatenate([r[rows, columns] for r in refs], 0)


def fetch(pairs, sems):
    copies = [pltpu.make_async_copy(a, b, sems.at[i]) for i, (a, b) in enumerate(pairs)]
    for c in copies:
        c.start()
    return copies


def pack_kernel(x_ref, bc_ref, dt_ref, z_ref, o_ref, f_ref, first, second, tail, fields, x, bc, dt, sems):
    k, width = x_ref.shape
    blocks = width // LANES
    part = k // blocks
    rows = f_ref.shape[0]
    copies = fetch(
        [
            (x_ref, x),
            (bc_ref, bc),
            (dt_ref, dt),
            (f_ref.at[rows - HALO :], tail),
            (z_ref, second.at[:k]),
            (o_ref, second.at[k:]),
            (f_ref, fields),
        ],
        sems,
    )
    for c in copies[:3]:
        c.wait()
    rest = jnp.zeros((part, width - LANES), BF16)
    for i in range(first.shape[0]):
        first[i, :k, :] = x[...]
        for j in range(blocks):
            first[i, k : k + part, j * LANES : (j + 1) * LANES] = bc[j * part : (j + 1) * part, :]
        first[i, k + part :, :LANES] = dt[...]
        first[i, k + part :, LANES:] = rest
    for c in copies[3:]:
        c.wait()


def source_kernel(order, f_ref, halo_ref, out):
    n = out.shape[1] // LANES
    for j in range(n):
        at = slice(j * LANES, (j + 1) * LANES)
        out[:HALO, at] = chunk(halo_ref, order[j])
        out[HALO:, at] = chunk(f_ref, order[j])


def project_kernel(
    src_ref, wa, wb, taps_x, taps_bc, bias_ref, rate_ref,
    x_out, bc_out, dt_out, cum_out, msg_out, pre, conv_x, conv_bc, bias, rate, sems,
):
    copies = fetch(
        [(taps_x, conv_x), (taps_bc, conv_bc), (bias_ref, bias), (rate_ref, rate)], sems
    )
    rows, width = x_out.shape
    heads = bias.shape[1]
    half = width // 2
    k = LANES
    n = 2 * wa.shape[0]
    blocks = width // LANES
    part = k // blocks
    shards = [r.at[i] for r in (wa, wb) for i in range(n // 2)]
    src = src_ref[...]
    first = HALO - conv_x.shape[0] + 1

    def conv(at, wide, taps):
        acc = taps[0:1, :] * pre[first : first + rows, at : at + wide]
        for i in range(1, conv_x.shape[0]):
            acc = acc + taps[i : i + 1, :] * pre[first + i : first + i + rows, at : at + wide]
        return silu(acc)

    w_dt = jnp.concatenate([r[i, k + part :, :LANES] for r in (wa, wb) for i in range(n // 2)], 1)
    dt_pre = dot_nt(src[HALO:], w_dt).astype(BF16).astype(F32)
    for c in copies:
        c.wait()
    step = jax.nn.softplus(dt_pre + bias[...])
    log_step = -jnp.exp(rate[...]) * step
    lower = (iota((rows, rows), 0) >= iota((rows, rows), 1)).astype(F32)
    cum = dot(lower, log_step, precision=HIGHEST)
    dt_out[...] = step
    cum_out[...] = cum
    last = cum[rows - 1 : rows, :]
    weight = spread(jnp.exp(last - cum) * step, width)

    w_bc = jnp.concatenate(
        [
            r[i, k : k + part, j * LANES : (j + 1) * LANES]
            for r in (wa, wb)
            for i in range(n // 2)
            for j in range(blocks)
        ],
        0,
    )
    pre[:, width:] = dot(src, w_bc).astype(BF16).astype(F32)
    bc = conv(width, LANES, conv_bc[...])
    bc_out[...] = bc.astype(BF16)
    left = iota((rows, LANES), 1) < LANES // 2
    b0 = jnp.where(left, bc, 0.0)
    b = (b0.astype(BF16), pltpu.roll(b0, LANES // 2, 1).astype(BF16))

    def end(at, q):
        pre[:, at : at + TILE] = (
            dot(src, stacked(shards, slice(0, k), slice(at, at + TILE))).astype(BF16).astype(F32)
        )
        x = conv(at, TILE, conv_x[:, at : at + TILE]).astype(BF16)
        x_out[:, at : at + TILE] = x
        xw = (x.astype(F32) * weight[:, at : at + TILE]).astype(BF16)
        return dot_tn(xw, b[q])

    for at in range(0, half, TILE):
        t = end(at, 0) + end(half + at, 1)
        msg_out[at // SUB : (at + TILE) // SUB, :SUB, :] = t.reshape(TILE // SUB, SUB, LANES).astype(BF16)
    pairs = heads // 2
    mine = iota((pairs, heads), 1) % pairs == iota((pairs, heads), 0)
    pick = (iota((heads, LANES), 1) // (LANES // 2) == iota((heads, LANES), 0) // pairs).astype(BF16)
    high, low = (dot(jnp.where(mine, v.astype(F32), 0.0).astype(BF16), pick) for v in halves(last))
    row = iota((SUB, LANES), 0)
    each = msg_out.shape[0] // pairs
    for j in range(pairs):
        tail = jnp.where(row == 0, high[j : j + 1, :], jnp.where(row == 1, low[j : j + 1, :], 0.0))
        for i in range(each):
            msg_out[j * each + i, SUB:, :] = tail.astype(BF16)


def within_kernel(x_ref, bc_ref, dt_ref, cum_ref, y_out):
    rows, _ = x_ref.shape
    heads = dt_ref.shape[1]
    state = bc_ref.shape[1] // 2
    scores = dot_nt(bc_ref[:, state:], bc_ref[:, :state])
    causal = iota((rows, rows), 0) >= iota((rows, rows), 1)
    cum = cum_ref[...]
    cum_t = cum.T
    dt_t = dt_ref[...].T
    left = iota((rows, LANES), 1) < LANES // 2
    for pair in range(heads // 2):
        w = []
        for h in (2 * pair, 2 * pair + 1):
            gap = jnp.where(causal, cum[:, h : h + 1] - cum_t[h : h + 1, :], -jnp.inf)
            w.append((jnp.exp(gap) * (scores * dt_t[h : h + 1, :])).astype(BF16))
        xp = x_ref[:, pair * LANES : (pair + 1) * LANES]
        zero = jnp.zeros_like(xp)
        both = jnp.concatenate([jnp.where(left, xp, zero), jnp.where(left, zero, xp)], 0)
        y_out[:, pair * LANES : (pair + 1) * LANES] = dot(jnp.concatenate(w, 1), both)


def bands_kernel(r_ref, e_out):
    carry = jnp.zeros(e_out.shape[1:], F32)
    for b in range(e_out.shape[0]):
        e_out[b] = carry.astype(BF16)
        tail = r_ref[b, SUB:, :].astype(F32)
        carry = jnp.exp(tail[0:1, :] + tail[1:2, :]) * carry + r_ref[b, :SUB, :].astype(F32)


def gate_kernel(near, order, f_ref, *refs):
    (out, w_out, w, sems) = refs[-4:]
    near_refs, (z_ref, o_ref), far_refs = refs[:near], refs[near : near + 2], refs[near + 2 : -4]
    k = z_ref.shape[0]
    n = len(far_refs) + 1 + near
    at = [pl.ds(i * k, k) for i in range(n)]
    copies = fetch(
        [(z_ref, w.at[at[0]])]
        + [(r.at[:k], w.at[at[i]]) for i, r in enumerate(far_refs, 1)]
        + [(o_ref, w_out.at[at[0]])]
        + [(r.at[k:], w_out.at[at[i]]) for i, r in enumerate(far_refs, 1)],
        sems,
    )
    for i, r in enumerate(near_refs, n - near):
        w_out[i * k : (i + 1) * k, :] = r[k:, :]
    src = ordered(f_ref, order, n)
    for c in copies[: n - near]:
        c.wait()
    for j in range(0, out.shape[1], TILE):
        cut = slice(j, j + TILE)
        tile = jnp.concatenate([w[: (n - near) * k, cut]] + [r[:k, cut] for r in near_refs], 0)
        out[:, cut] = dot(src, tile).astype(BF16)
    for c in copies[n - near :]:
        c.wait()


def finish_kernel(order, y_ref, in_ref, bc_ref, cum_ref, gate_ref, gain, w, out, hidden):
    rows, width = y_ref.shape
    half = width // 2
    bc = bc_ref[...].astype(F32)
    left = iota((rows, LANES), 1) < LANES // 2
    c1 = jnp.where(left, 0.0, bc)
    c = (pltpu.roll(c1, LANES // 2, 1).astype(BF16), c1.astype(BF16))
    grown = spread(jnp.exp(cum_ref[...]), width)
    square = jnp.zeros((rows, 1), F32)
    parts = []
    for at in range(0, width, TILE):
        inner = in_ref[at % half : at % half + TILE, :]
        y = y_ref[:, at : at + TILE] + dot_nt(c[at // half], inner) * grown[:, at : at + TILE]
        g = y * silu(gate_ref[:, at : at + TILE].astype(F32))
        square = square + jnp.sum(g * g, -1, keepdims=True)
        parts.append(g)
    scale = lax.rsqrt(square / width + EPS)
    for i, at in enumerate(range(0, width, TILE)):
        hidden[:, at : at + TILE] = (parts[i] * scale * gain[:, at : at + TILE]).astype(BF16)
    src = ordered(hidden, order, width // LANES)
    for at in range(0, out.shape[1], TILE):
        out[:, at : at + TILE] = dot(src, w[:, at : at + TILE]).astype(BF16)


def call(body, outs, args, smem=0, hbm=0, scratch=(), flops=0):
    vmem = pl.BlockSpec(memory_space=pltpu.VMEM)
    specs = (
        [pl.BlockSpec(memory_space=pltpu.SMEM)] * smem
        + [vmem] * (len(args) - smem - hbm)
        + [pl.BlockSpec(memory_space=pltpu.MemorySpace.HBM)] * hbm
    )
    args = [
        pltpu.with_memory_space_constraint(a, pltpu.MemorySpace.HBM) if i >= len(args) - hbm else a
        for i, a in enumerate(args)
    ]
    scratch = list(scratch) + ([pltpu.SemaphoreType.DMA((2 * hbm,))] if hbm else [])
    nbytes = sum(a.size * a.dtype.itemsize for a in args)
    return pl.pallas_call(
        body,
        out_shape=outs,
        in_specs=specs,
        out_specs=jax.tree.map(lambda _: vmem, outs),
        scratch_shapes=scratch,
        compiler_params=pltpu.CompilerParams(vmem_limit_bytes=16 * 2**20),
        cost_estimate=pl.CostEstimate(flops=flops, bytes_accessed=nbytes, transcendentals=0),
    )(*args)


def local(
    fields, proj_x, proj_z, proj_bc, proj_dt, conv_x, conv_bc, dt_bias, log_rate, norm_gain, proj_out
):
    rows, _, depth = fields.shape
    heads = log_rate.shape[0]
    width = proj_x.shape[1]
    state = proj_bc.shape[1] // 2
    n_x = lax.axis_size("x")
    bands = lax.axis_size(LAT)
    f = fields.reshape(rows, depth)
    sds = jax.ShapeDtypeStruct

    k = proj_x.shape[0]
    x_at, c_at = lax.axis_index("x"), lax.axis_index("c")
    each = jnp.arange(2 * n_x)
    order = each % n_x * 2 + (c_at + each // n_x) % 2
    late = jnp.array([0, 1, 3, 2, 4, 6, 5, 7])
    order2 = (x_at - late + 2 * n_x) % n_x * 2 + (c_at + late // n_x) % 2
    first, second, tail, f = call(
        pack_kernel,
        (
            sds((n_x, k + 2 * k * LANES // width, width), BF16),
            sds((2 * k, width), BF16),
            sds((HALO, depth), BF16),
            sds((rows, depth), BF16),
        ),
        [proj_x, proj_bc, proj_dt.T, proj_z, proj_out, f],
        hbm=6,
        scratch=[
            pltpu.VMEM(proj_x.shape, BF16),
            pltpu.VMEM(proj_bc.shape, BF16),
            pltpu.VMEM(proj_dt.shape[::-1], BF16),
        ],
    )

    def across(block):
        return lax.ppermute(block, "c", [(0, 1), (1, 0)])

    w1a = lax.all_to_all(first, "x", 0, 0)
    halo = lax.ppermute(tail, LAT, [(i, i + 1) for i in range(bands - 1)])
    w2a, w2b = [second], [across(second)]
    src = call(
        source_kernel, sds((HALO + rows, depth), BF16), [order, f, halo], smem=1, flops=10**6
    )
    w1a, src, second, order2 = lax.optimization_barrier((w1a, src, second, order2))
    w1b = across(w1a)
    for d in range(1, n_x):
        w2a.append(lax.ppermute(second, "x", [(i, (i + d) % n_x) for i in range(n_x)]))
    for d in range(1, n_x):
        w2b.append(across(w2a[d]))

    x_act, bc_act, step, cum, msg = call(
        project_kernel,
        (
            sds((rows, width), BF16),
            sds((rows, 2 * state), BF16),
            sds((rows, heads), F32),
            sds((rows, heads), F32),
            sds((bands, 2 * SUB, LANES), BF16),
        ),
        [src, w1a, w1b, conv_x, conv_bc, dt_bias[None], log_rate[None]],
        hbm=4,
        scratch=[pltpu.VMEM((HALO + rows, width + 2 * state), F32)]
        + [pltpu.VMEM(a.shape, F32) for a in (conv_x, conv_bc, dt_bias[None], log_rate[None])],
        flops=2 * rows * depth * (width + 2 * LANES),
    )
    got = lax.all_to_all(msg, LAT, 0, 0)
    y = call(
        within_kernel,
        sds((rows, width), F32),
        [x_act, bc_act, step, cum],
        flops=2 * rows * rows * width * 2,
    )
    entering = call(
        bands_kernel, sds((bands, SUB, LANES), BF16), [got], flops=bands * SUB * LANES * 100
    )
    incoming = lax.all_to_all(entering, LAT, 0, 0)
    incoming = incoming.reshape(bands * SUB, LANES)
    near = []
    gate, w_out = call(
        functools.partial(gate_kernel, len(near)),
        (sds((rows, width), BF16), sds((width, depth), BF16)),
        [order2, f, *near, proj_z, proj_out, w2a[1], w2a[3], w2a[2], w2b[0], w2b[2], w2b[1], w2b[3]],
        smem=1,
        hbm=9,
        scratch=[pltpu.VMEM((depth, width), BF16)],
        flops=2 * rows * depth * width,
    )
    out = call(
        finish_kernel,
        sds((rows, depth), BF16),
        [order2, y, incoming, bc_act, cum, gate, norm_gain[None], w_out],
        smem=1,
        scratch=[pltpu.VMEM((rows, width), BF16)],
        flops=2 * rows * depth * width,
    )
    return out.reshape(rows, 1, depth)


def solution(mesh):
    finer = Mesh(mesh.devices.reshape(8, 8, 4, 2), ("z", "y", "x", "c"))
    lat, lon = P(LAT, ("x", "c"), None), P(("x", "c"), None)
    return jax.shard_map(
        local,
        mesh=finer,
        in_specs=(lat, lon, lon, lon, lon, P(), P(), P(), P(), P(), lon),
        out_specs=lat,
        check_vma=False,
    )
```

```python
import functools

import jax
import jax.numpy as jnp
from jax import lax
from jax.experimental import pallas as pl
from jax.experimental.pallas import tpu as pltpu
from jax.sharding import Mesh
from jax.sharding import PartitionSpec as P


LAT = ("z", "y")
EPS = 1e-05
HIGHEST = lax.Precision.HIGHEST
F32 = jnp.float32
BF16 = jnp.bfloat16
HALO = 16
LANES = 128
SUB = 8
TILE = 256


def dot(a, b, **kw):
    return jnp.dot(a, b, preferred_element_type=F32, **kw)


def dot_nt(a, b):
    return lax.dot_general(a, b, (((1,), (1,)), ((), ())), preferred_element_type=F32)


def dot_tn(a, b):
    return lax.dot_general(a, b, (((0,), (0,)), ((), ())), preferred_element_type=F32)


def iota(shape, dim):
    return lax.broadcasted_iota(jnp.int32, shape, dim)


def silu(v):
    return v / (1.0 + jnp.exp(-v))


def halves(v):
    high = v.astype(BF16)
    return high, (v - high.astype(F32)).astype(BF16)


def spread(v, width):
    heads = v.shape[1]
    shape = (heads, width)
    pick = (iota(shape, 1) // (width // heads) == iota(shape, 0)).astype(BF16)
    high, low = halves(v)
    return dot(high, pick) + dot(low, pick)


def chunk(ref, index):
    return ref[:, pl.ds(pl.multiple_of(index * LANES, LANES), LANES)]


def ordered(ref, order, n):
    return jnp.concatenate([chunk(ref, order[j]) for j in range(n)], 1)


def stacked(refs, rows, columns):
    return jnp.concatenate([r[rows, columns] for r in refs], 0)


def fetch(pairs, sems):
    copies = [pltpu.make_async_copy(a, b, sems.at[i]) for i, (a, b) in enumerate(pairs)]
    for c in copies:
        c.start()
    return copies


def pack_kernel(x_ref, bc_ref, dt_ref, f_ref, first, tail, x, bc, dt, sems):
    k, width = x_ref.shape
    blocks = width // LANES
    part = k // blocks
    copies = fetch(
        [(x_ref, x), (bc_ref, bc), (dt_ref, dt), (f_ref.at[f_ref.shape[0] - HALO :], tail)], sems
    )
    for c in copies:
        c.wait()
    rest = jnp.zeros((part, width - LANES), BF16)
    for i in range(first.shape[0]):
        first[i, :k, :] = x[...]
        for j in range(blocks):
            first[i, k : k + part, j * LANES : (j + 1) * LANES] = bc[j * part : (j + 1) * part, :]
        first[i, k + part :, :LANES] = dt[...]
        first[i, k + part :, LANES:] = rest


def source_kernel(order, halo_ref, *refs):
    z_ref, o_ref, f_ref = refs[:3]
    small_refs = refs[3:7]
    out, second, fields = refs[7:10]
    small, sems = refs[10:14], refs[14]
    k = z_ref.shape[0]
    copies = fetch(
        [(f_ref, fields), (z_ref, second.at[:k]), (o_ref, second.at[k:])]
        + list(zip(small_refs, small)),
        sems,
    )
    n = out.shape[1] // LANES
    copies[0].wait()
    for j in range(n):
        at = slice(j * LANES, (j + 1) * LANES)
        out[:HALO, at] = chunk(halo_ref, order[j])
        out[HALO:, at] = chunk(fields, order[j])
    for c in copies[1:]:
        c.wait()


def tail_rows(high, low):
    row = iota((SUB, LANES), 0)
    return jnp.where(row == 0, high, jnp.where(row == 1, low, 0.0)).astype(BF16)


def part_of(ref, b):
    size = ref.shape[1] - SUB
    tail = ref[b, size:, :].astype(F32)
    return ref[b, :size, :].astype(F32), tail[0:1, :] + tail[1:2, :]


def project_kernel(
    src_ref, wa, wb, conv_x, conv_bc, bias, rate, x_out, bc_out, dt_out, cum_out, msg_out, pre
):
    rows, width = x_out.shape
    heads = bias.shape[1]
    per = width // heads
    half = width // 2
    k = LANES
    n = 2 * wa.shape[0]
    blocks = width // LANES
    part = k // blocks
    shards = [r.at[i] for r in (wa, wb) for i in range(n // 2)]
    src = src_ref[...]
    first = HALO - conv_x.shape[0] + 1

    def conv(at, wide, taps):
        acc = taps[0:1, :] * pre[first : first + rows, at : at + wide]
        for i in range(1, conv_x.shape[0]):
            acc = acc + taps[i : i + 1, :] * pre[first + i : first + i + rows, at : at + wide]
        return silu(acc)

    w_dt = jnp.concatenate([r[i, k + part :, :LANES] for r in (wa, wb) for i in range(n // 2)], 1)
    dt_pre = dot_nt(src[HALO:], w_dt).astype(BF16).astype(F32)
    step = jax.nn.softplus(dt_pre + bias[...])
    log_step = -jnp.exp(rate[...]) * step
    lower = (iota((rows, rows), 0) >= iota((rows, rows), 1)).astype(F32)
    cum = dot(lower, log_step, precision=HIGHEST)
    dt_out[...] = step
    cum_out[...] = cum
    last = cum[rows - 1 : rows, :]
    weight = spread(jnp.exp(last - cum) * step, width)

    w_bc = jnp.concatenate(
        [
            r[i, k : k + part, j * LANES : (j + 1) * LANES]
            for r in (wa, wb)
            for i in range(n // 2)
            for j in range(blocks)
        ],
        0,
    )
    pre[:, width:] = dot(src, w_bc).astype(BF16).astype(F32)
    bc = conv(width, LANES, conv_bc[...])
    bc_out[...] = bc.astype(BF16)
    left = iota((rows, LANES), 1) < LANES // 2
    b0 = jnp.where(left, bc, 0.0)
    b = (b0.astype(BF16), pltpu.roll(b0, LANES // 2, 1).astype(BF16))

    def end(at, q):
        pre[:, at : at + TILE] = (
            dot(src, stacked(shards, slice(0, k), slice(at, at + TILE))).astype(BF16).astype(F32)
        )
        x = conv(at, TILE, conv_x[:, at : at + TILE]).astype(BF16)
        x_out[:, at : at + TILE] = x
        xw = (x.astype(F32) * weight[:, at : at + TILE]).astype(BF16)
        return dot_tn(xw, b[q])

    for at in range(0, half, TILE):
        t = end(at, 0) + end(half + at, 1)
        for i in range(0, TILE, per):
            msg_out[(at + i) // per, :per, :] = t[i : i + per].astype(BF16)
    pairs = heads // 2
    mine = iota((pairs, heads), 1) % pairs == iota((pairs, heads), 0)
    pick = (iota((heads, LANES), 1) // (LANES // 2) == iota((heads, LANES), 0) // pairs).astype(BF16)
    high, low = (dot(jnp.where(mine, v.astype(F32), 0.0).astype(BF16), pick) for v in halves(last))
    for j in range(pairs):
        msg_out[j, per:, :] = tail_rows(high[j : j + 1, :], low[j : j + 1, :])


def within_kernel(x_ref, bc_ref, dt_ref, cum_ref, y_out):
    rows, _ = x_ref.shape
    heads = dt_ref.shape[1]
    state = bc_ref.shape[1] // 2
    scores = dot_nt(bc_ref[:, state:], bc_ref[:, :state])
    causal = iota((rows, rows), 0) >= iota((rows, rows), 1)
    cum = cum_ref[...]
    cum_t = cum.T
    dt_t = dt_ref[...].T
    left = iota((rows, LANES), 1) < LANES // 2
    for pair in range(heads // 2):
        w = []
        for h in (2 * pair, 2 * pair + 1):
            gap = jnp.where(causal, cum[:, h : h + 1] - cum_t[h : h + 1, :], -jnp.inf)
            w.append((jnp.exp(gap) * (scores * dt_t[h : h + 1, :])).astype(BF16))
        xp = x_ref[:, pair * LANES : (pair + 1) * LANES]
        zero = jnp.zeros_like(xp)
        both = jnp.concatenate([jnp.where(left, xp, zero), jnp.where(left, zero, xp)], 0)
        y_out[:, pair * LANES : (pair + 1) * LANES] = dot(jnp.concatenate(w, 1), both)


def row_kernel(r_ref, before, decay, msg_out):
    state = jnp.zeros(before.shape[1:], F32)
    total = jnp.zeros((1, LANES), F32)
    for b in range(r_ref.shape[0]):
        before[b] = state
        decay[b : b + 1, :] = total
        own, step = part_of(r_ref, b)
        state = jnp.exp(step) * state + own
        total = total + step
    high, low = (v.astype(F32) for v in halves(total))
    tail = tail_rows(high, low)
    for z in range(msg_out.shape[0]):
        msg_out[z, : state.shape[0], :] = state.astype(BF16)
        msg_out[z, state.shape[0] :, :] = tail


def enter_kernel(place, r_ref, before, decay, e_out):
    state = jnp.zeros(before.shape[1:], F32)
    for z in range(r_ref.shape[0]):
        own, step = part_of(r_ref, z)
        state = jnp.where(z < place[0], jnp.exp(step) * state + own, state)
    for b in range(e_out.shape[0]):
        e_out[b] = (before[b] + jnp.exp(decay[b : b + 1, :]) * state).astype(BF16)


def gate_kernel(near, order, f_ref, *refs):
    (out, w_out, w, sems) = refs[-4:]
    near_refs, (z_ref, o_ref), far_refs = refs[:near], refs[near : near + 2], refs[near + 2 : -4]
    k = z_ref.shape[0]
    n = len(far_refs) + 1 + near
    at = [pl.ds(i * k, k) for i in range(n)]
    copies = fetch(
        [(z_ref, w.at[at[0]])]
        + [(r.at[:k], w.at[at[i]]) for i, r in enumerate(far_refs, 1)]
        + [(o_ref, w_out.at[at[0]])]
        + [(r.at[k:], w_out.at[at[i]]) for i, r in enumerate(far_refs, 1)],
        sems,
    )
    for i, r in enumerate(near_refs, n - near):
        w_out[i * k : (i + 1) * k, :] = r[k:, :]
    src = ordered(f_ref, order, n)
    for c in copies[: n - near]:
        c.wait()
    for j in range(0, out.shape[1], TILE):
        cut = slice(j, j + TILE)
        tile = jnp.concatenate([w[: (n - near) * k, cut]] + [r[:k, cut] for r in near_refs], 0)
        out[:, cut] = dot(src, tile).astype(BF16)
    for c in copies[n - near :]:
        c.wait()


def finish_kernel(order, y_ref, in_ref, bc_ref, cum_ref, gate_ref, gain, w, out, hidden):
    rows, width = y_ref.shape
    half = width // 2
    bc = bc_ref[...].astype(F32)
    left = iota((rows, LANES), 1) < LANES // 2
    c1 = jnp.where(left, 0.0, bc)
    c = (pltpu.roll(c1, LANES // 2, 1).astype(BF16), c1.astype(BF16))
    grown = spread(jnp.exp(cum_ref[...]), width)
    square = jnp.zeros((rows, 1), F32)
    parts = []
    for at in range(0, width, TILE):
        inner = in_ref[at % half : at % half + TILE, :]
        y = y_ref[:, at : at + TILE] + dot_nt(c[at // half], inner) * grown[:, at : at + TILE]
        g = y * silu(gate_ref[:, at : at + TILE].astype(F32))
        square = square + jnp.sum(g * g, -1, keepdims=True)
        parts.append(g)
    scale = lax.rsqrt(square / width + EPS)
    for i, at in enumerate(range(0, width, TILE)):
        hidden[:, at : at + TILE] = (parts[i] * scale * gain[:, at : at + TILE]).astype(BF16)
    src = ordered(hidden, order, width // LANES)
    for at in range(0, out.shape[1], TILE):
        out[:, at : at + TILE] = dot(src, w[:, at : at + TILE]).astype(BF16)


def call(body, outs, args, smem=0, hbm=0, scratch=(), flops=0):
    vmem = pl.BlockSpec(memory_space=pltpu.VMEM)
    specs = (
        [pl.BlockSpec(memory_space=pltpu.SMEM)] * smem
        + [vmem] * (len(args) - smem - hbm)
        + [pl.BlockSpec(memory_space=pltpu.MemorySpace.HBM)] * hbm
    )
    args = [
        pltpu.with_memory_space_constraint(a, pltpu.MemorySpace.HBM) if i >= len(args) - hbm else a
        for i, a in enumerate(args)
    ]
    scratch = list(scratch) + ([pltpu.SemaphoreType.DMA((2 * hbm,))] if hbm else [])
    nbytes = sum(a.size * a.dtype.itemsize for a in args)
    return pl.pallas_call(
        body,
        out_shape=outs,
        in_specs=specs,
        out_specs=jax.tree.map(lambda _: vmem, outs),
        scratch_shapes=scratch,
        compiler_params=pltpu.CompilerParams(vmem_limit_bytes=16 * 2**20),
        cost_estimate=pl.CostEstimate(flops=flops, bytes_accessed=nbytes, transcendentals=0),
    )(*args)


def local(
    fields, proj_x, proj_z, proj_bc, proj_dt, conv_x, conv_bc, dt_bias, log_rate, norm_gain, proj_out
):
    rows, _, depth = fields.shape
    heads = log_rate.shape[0]
    width = proj_x.shape[1]
    state = proj_bc.shape[1] // 2
    n_x = lax.axis_size("x")
    n_z, n_y = lax.axis_size("z"), lax.axis_size("y")
    bands = n_z * n_y
    f = fields.reshape(rows, depth)
    sds = jax.ShapeDtypeStruct

    k = proj_x.shape[0]
    x_at, c_at = lax.axis_index("x"), lax.axis_index("c")
    each = jnp.arange(2 * n_x)
    order = each % n_x * 2 + (c_at + each // n_x) % 2
    late = jnp.array([0, 1, 3, 2, 4, 6, 5, 7])
    order2 = (x_at - late + 2 * n_x) % n_x * 2 + (c_at + late // n_x) % 2
    first, tail = call(
        pack_kernel,
        (sds((n_x, k + 2 * k * LANES // width, width), BF16), sds((HALO, depth), BF16)),
        [proj_x, proj_bc, proj_dt.T, f],
        hbm=4,
        scratch=[
            pltpu.VMEM(proj_x.shape, BF16),
            pltpu.VMEM(proj_bc.shape, BF16),
            pltpu.VMEM(proj_dt.shape[::-1], BF16),
        ],
    )

    def across(block):
        return lax.ppermute(block, "c", [(0, 1), (1, 0)])

    w1a = lax.all_to_all(first, "x", 0, 0)
    halo = lax.ppermute(tail, LAT, [(i, i + 1) for i in range(bands - 1)])
    small = [conv_x, conv_bc, dt_bias[None], log_rate[None]]
    src, second, f, *small = call(
        source_kernel,
        [sds((HALO + rows, depth), BF16), sds((2 * k, width), BF16), sds((rows, depth), BF16)]
        + [sds(a.shape, F32) for a in small],
        [order, halo, proj_z, proj_out, f, *small],
        smem=1,
        hbm=7,
        flops=10**6,
    )
    w2a, w2b = [second], [across(second)]
    w1a, src, second, order2, w2b[0] = lax.optimization_barrier(
        (w1a, src, second, order2, w2b[0])
    )
    w1b = across(w1a)
    for d in range(1, n_x):
        w2a.append(lax.ppermute(second, "x", [(i, (i + d) % n_x) for i in range(n_x)]))
    for d in range(1, n_x):
        w2b.append(across(w2a[d]))

    x_act, bc_act, step, cum, msg = call(
        project_kernel,
        (
            sds((rows, width), BF16),
            sds((rows, 2 * state), BF16),
            sds((rows, heads), F32),
            sds((rows, heads), F32),
            sds((n_y, width // heads + SUB, LANES), BF16),
        ),
        [src, w1a, w1b, *small],
        scratch=[pltpu.VMEM((HALO + rows, width + 2 * state), F32)],
        flops=2 * rows * depth * (width + 2 * LANES),
    )
    got = lax.all_to_all(msg, "y", 0, 0)
    y = call(
        within_kernel,
        sds((rows, width), F32),
        [x_act, bc_act, step, cum],
        flops=2 * rows * rows * width * 2,
    )
    per = width // heads
    before, decay, msg = call(
        row_kernel,
        (
            sds((n_y, per, LANES), F32),
            sds((n_y, LANES), F32),
            sds((n_z, per + SUB, LANES), BF16),
        ),
        [got],
        flops=10**6,
    )
    got = lax.all_to_all(msg, "z", 0, 0)
    entering = call(
        enter_kernel,
        sds((n_y, per, LANES), BF16),
        [lax.axis_index("z")[None], got, before, decay],
        smem=1,
        flops=10**6,
    )
    incoming = lax.all_to_all(entering, "y", 0, 0)
    incoming = incoming.reshape(width // 2, LANES)
    near = []
    gate, w_out = call(
        functools.partial(gate_kernel, len(near)),
        (sds((rows, width), BF16), sds((width, depth), BF16)),
        [order2, f, *near, proj_z, proj_out, w2a[1], w2a[3], w2a[2], w2b[0], w2b[2], w2b[1], w2b[3]],
        smem=1,
        hbm=9,
        scratch=[pltpu.VMEM((depth, width), BF16)],
        flops=2 * rows * depth * width,
    )
    out = call(
        finish_kernel,
        sds((rows, depth), BF16),
        [order2, y, incoming, bc_act, cum, gate, norm_gain[None], w_out],
        smem=1,
        scratch=[pltpu.VMEM((rows, width), BF16)],
        flops=2 * rows * depth * width,
    )
    return out.reshape(rows, 1, depth)


def solution(mesh):
    finer = Mesh(mesh.devices.reshape(8, 8, 4, 2), ("z", "y", "x", "c"))
    lat, lon = P(LAT, ("x", "c"), None), P(("x", "c"), None)
    return jax.shard_map(
        local,
        mesh=finer,
        in_specs=(lat, lon, lon, lon, lon, P(), P(), P(), P(), P(), lon),
        out_specs=lat,
        check_vma=False,
    )
```

```python
import jax
import jax.numpy as jnp
from jax import lax
from jax.experimental import pallas as pl
from jax.experimental.pallas import tpu as pltpu
from jax.sharding import Mesh
from jax.sharding import PartitionSpec as P


LAT = ("z", "y")
EPS = 1e-05
HIGHEST = lax.Precision.HIGHEST
F32 = jnp.float32
BF16 = jnp.bfloat16
HALO = 16
LANES = 128
SUB = 8
TILE = 256
HELD = type(pltpu.HBM((8, 128), jnp.bfloat16))


def dot(a, b, **kw):
    return jnp.dot(a, b, preferred_element_type=F32, **kw)


def dot_nt(a, b):
    return lax.dot_general(a, b, (((1,), (1,)), ((), ())), preferred_element_type=F32)


def dot_tn(a, b):
    return lax.dot_general(a, b, (((0,), (0,)), ((), ())), preferred_element_type=F32)


def iota(shape, dim):
    return lax.broadcasted_iota(jnp.int32, shape, dim)


def silu(v):
    return v / (1.0 + jnp.exp(-v))


def halves(v):
    high = v.astype(BF16)
    return high, (v - high.astype(F32)).astype(BF16)


def spread(v, width):
    heads = v.shape[1]
    shape = (heads, width)
    pick = (iota(shape, 1) // (width // heads) == iota(shape, 0)).astype(BF16)
    high, low = halves(v)
    return dot(high, pick) + dot(low, pick)


def chunk(ref, index):
    return ref[:, pl.ds(pl.multiple_of(index * LANES, LANES), LANES)]


def ordered(ref, order, n):
    return jnp.concatenate([chunk(ref, order[j]) for j in range(n)], 1)


def stacked(refs, rows, columns):
    return jnp.concatenate([r[rows, columns] for r in refs], 0)


def fetch(pairs, sems):
    copies = [pltpu.make_async_copy(a, b, sems.at[i]) for i, (a, b) in enumerate(pairs)]
    for c in copies:
        c.start()
    return copies


def pack_kernel(x_ref, bc_ref, dt_ref, f_ref, first, tail, x, bc, dt, sems):
    k, width = x_ref.shape
    blocks = width // LANES
    part = k // blocks
    copies = fetch(
        [(x_ref, x), (bc_ref, bc), (dt_ref, dt), (f_ref.at[f_ref.shape[0] - HALO :], tail)], sems
    )
    for c in copies:
        c.wait()
    rest = jnp.zeros((part, width - LANES), BF16)
    for i in range(first.shape[0]):
        first[i, :k, :] = x[...]
        for j in range(blocks):
            first[i, k : k + part, j * LANES : (j + 1) * LANES] = bc[j * part : (j + 1) * part, :]
        first[i, k + part :, :LANES] = dt[...]
        first[i, k + part :, LANES:] = rest


def source_kernel(order, halo_ref, *refs):
    z_ref, o_ref, f_ref = refs[:3]
    small_refs = refs[3:7]
    out, second, fields = refs[7:10]
    small, sems = refs[10:14], refs[14]
    k = z_ref.shape[0]
    copies = fetch(
        [(f_ref, fields), (z_ref, second.at[:k]), (o_ref, second.at[k:])]
        + list(zip(small_refs, small)),
        sems,
    )
    n = out.shape[1] // LANES
    copies[0].wait()
    for j in range(n):
        at = slice(j * LANES, (j + 1) * LANES)
        out[:HALO, at] = chunk(halo_ref, order[j])
        out[HALO:, at] = chunk(fields, order[j])
    for c in copies[1:]:
        c.wait()


def tail_rows(high, low):
    row = iota((SUB, LANES), 0)
    return jnp.where(row == 0, high, jnp.where(row == 1, low, 0.0)).astype(BF16)


def part_of(ref, b):
    size = ref.shape[1] - SUB
    tail = ref[b, size:, :].astype(F32)
    return ref[b, :size, :].astype(F32), tail[0:1, :] + tail[1:2, :]


def project_kernel(
    src_ref, wa, wb, conv_x, conv_bc, bias, rate, x_out, bc_out, dt_out, cum_out, msg_out, pre
):
    rows, width = x_out.shape
    heads = bias.shape[1]
    per = width // heads
    half = width // 2
    k = LANES
    n = 2 * wa.shape[0]
    blocks = width // LANES
    part = k // blocks
    shards = [r.at[i] for r in (wa, wb) for i in range(n // 2)]
    src = src_ref[...]
    first = HALO - conv_x.shape[0] + 1

    def conv(at, wide, taps):
        acc = taps[0:1, :] * pre[first : first + rows, at : at + wide]
        for i in range(1, conv_x.shape[0]):
            acc = acc + taps[i : i + 1, :] * pre[first + i : first + i + rows, at : at + wide]
        return silu(acc)

    w_dt = jnp.concatenate([r[i, k + part :, :LANES] for r in (wa, wb) for i in range(n // 2)], 1)
    dt_pre = dot_nt(src[HALO:], w_dt).astype(BF16).astype(F32)
    step = jax.nn.softplus(dt_pre + bias[...])
    log_step = -jnp.exp(rate[...]) * step
    lower = (iota((rows, rows), 0) >= iota((rows, rows), 1)).astype(F32)
    cum = dot(lower, log_step, precision=HIGHEST)
    dt_out[...] = step
    cum_out[...] = cum
    last = cum[rows - 1 : rows, :]
    weight = spread(jnp.exp(last - cum) * step, width)

    w_bc = jnp.concatenate(
        [
            r[i, k : k + part, j * LANES : (j + 1) * LANES]
            for r in (wa, wb)
            for i in range(n // 2)
            for j in range(blocks)
        ],
        0,
    )
    pre[:, width:] = dot(src, w_bc).astype(BF16).astype(F32)
    bc = conv(width, LANES, conv_bc[...])
    bc_out[...] = bc.astype(BF16)
    left = iota((rows, LANES), 1) < LANES // 2
    b0 = jnp.where(left, bc, 0.0)
    b = (b0.astype(BF16), pltpu.roll(b0, LANES // 2, 1).astype(BF16))

    def end(at, q):
        pre[:, at : at + TILE] = (
            dot(src, stacked(shards, slice(0, k), slice(at, at + TILE))).astype(BF16).astype(F32)
        )
        x = conv(at, TILE, conv_x[:, at : at + TILE]).astype(BF16)
        x_out[:, at : at + TILE] = x
        xw = (x.astype(F32) * weight[:, at : at + TILE]).astype(BF16)
        return dot_tn(xw, b[q])

    for at in range(0, half, TILE):
        t = end(at, 0) + end(half + at, 1)
        for i in range(0, TILE, per):
            msg_out[(at + i) // per, :per, :] = t[i : i + per].astype(BF16)
    pairs = heads // 2
    mine = iota((pairs, heads), 1) % pairs == iota((pairs, heads), 0)
    pick = (iota((heads, LANES), 1) // (LANES // 2) == iota((heads, LANES), 0) // pairs).astype(BF16)
    high, low = (dot(jnp.where(mine, v.astype(F32), 0.0).astype(BF16), pick) for v in halves(last))
    for j in range(pairs):
        msg_out[j, per:, :] = tail_rows(high[j : j + 1, :], low[j : j + 1, :])


def within_kernel(x_ref, bc_ref, dt_ref, cum_ref, y_out):
    rows, _ = x_ref.shape
    heads = dt_ref.shape[1]
    state = bc_ref.shape[1] // 2
    scores = dot_nt(bc_ref[:, state:], bc_ref[:, :state])
    causal = iota((rows, rows), 0) >= iota((rows, rows), 1)
    cum = cum_ref[...]
    cum_t = cum.T
    dt_t = dt_ref[...].T
    left = iota((rows, LANES), 1) < LANES // 2
    for pair in range(heads // 2):
        w = []
        for h in (2 * pair, 2 * pair + 1):
            gap = jnp.where(causal, cum[:, h : h + 1] - cum_t[h : h + 1, :], -jnp.inf)
            w.append((jnp.exp(gap) * (scores * dt_t[h : h + 1, :])).astype(BF16))
        xp = x_ref[:, pair * LANES : (pair + 1) * LANES]
        zero = jnp.zeros_like(xp)
        both = jnp.concatenate([jnp.where(left, xp, zero), jnp.where(left, zero, xp)], 0)
        y_out[:, pair * LANES : (pair + 1) * LANES] = dot(jnp.concatenate(w, 1), both)


def stack_kernel(*refs):
    parts, (out, sems) = refs[:-2], refs[-2:]
    size = parts[0].shape[0]
    for c in fetch([(r, out.at[pl.ds(i * size, size)]) for i, r in enumerate(parts)], sems):
        c.wait()


def row_kernel(r_ref, before, decay, msg_out):
    state = jnp.zeros(before.shape[1:], F32)
    total = jnp.zeros((1, LANES), F32)
    for b in range(r_ref.shape[0]):
        before[b] = state
        decay[b : b + 1, :] = total
        own, step = part_of(r_ref, b)
        state = jnp.exp(step) * state + own
        total = total + step
    high, low = (v.astype(F32) for v in halves(total))
    tail = tail_rows(high, low)
    for z in range(msg_out.shape[0]):
        msg_out[z, : state.shape[0], :] = state.astype(BF16)
        msg_out[z, state.shape[0] :, :] = tail


def enter_kernel(place, r_ref, before, decay, e_out):
    state = jnp.zeros(before.shape[1:], F32)
    for z in range(r_ref.shape[0]):
        own, step = part_of(r_ref, z)
        state = jnp.where(z < place[0], jnp.exp(step) * state + own, state)
    for b in range(e_out.shape[0]):
        e_out[b] = (before[b] + jnp.exp(decay[b : b + 1, :]) * state).astype(BF16)


def gate_kernel(order, f_ref, z_ref, o_ref, mine, other, others, out, w_out, w, sems):
    k, width = z_ref.shape
    n = w.shape[0] // k
    shards = [(z_ref, o_ref)]
    for ref in (mine, other, others):
        for i in range(0, ref.shape[0], 2 * k):
            shards.append((ref.at[pl.ds(i, k)], ref.at[pl.ds(i + k, k)]))
    copies = fetch(
        [(s[0], w.at[pl.ds(i * k, k)]) for i, s in enumerate(shards)]
        + [(s[1], w_out.at[pl.ds(i * k, k)]) for i, s in enumerate(shards)],
        sems,
    )
    src = ordered(f_ref, order, n)
    for c in copies[:n]:
        c.wait()
    for at in range(0, width, TILE):
        out[:, at : at + TILE] = dot(src, w[:, at : at + TILE]).astype(BF16)
    for c in copies[n:]:
        c.wait()


def finish_kernel(order, y_ref, in_ref, bc_ref, cum_ref, gate_ref, gain, w, out, hidden):
    rows, width = y_ref.shape
    half = width // 2
    bc = bc_ref[...].astype(F32)
    left = iota((rows, LANES), 1) < LANES // 2
    c1 = jnp.where(left, 0.0, bc)
    c = (pltpu.roll(c1, LANES // 2, 1).astype(BF16), c1.astype(BF16))
    grown = spread(jnp.exp(cum_ref[...]), width)
    square = jnp.zeros((rows, 1), F32)
    parts = []
    for at in range(0, width, TILE):
        inner = in_ref[at % half : at % half + TILE, :]
        y = y_ref[:, at : at + TILE] + dot_nt(c[at // half], inner) * grown[:, at : at + TILE]
        g = y * silu(gate_ref[:, at : at + TILE].astype(F32))
        square = square + jnp.sum(g * g, -1, keepdims=True)
        parts.append(g)
    scale = lax.rsqrt(square / width + EPS)
    for i, at in enumerate(range(0, width, TILE)):
        hidden[:, at : at + TILE] = (parts[i] * scale * gain[:, at : at + TILE]).astype(BF16)
    src = ordered(hidden, order, width // LANES)
    for at in range(0, out.shape[1], TILE):
        out[:, at : at + TILE] = dot(src, w[:, at : at + TILE]).astype(BF16)


def call(body, outs, args, smem=0, hbm=0, scratch=(), flops=0):
    vmem = pl.BlockSpec(memory_space=pltpu.VMEM)
    specs = (
        [pl.BlockSpec(memory_space=pltpu.SMEM)] * smem
        + [vmem] * (len(args) - smem - hbm)
        + [pl.BlockSpec(memory_space=pltpu.MemorySpace.HBM)] * hbm
    )
    args = [
        pltpu.with_memory_space_constraint(a, pltpu.MemorySpace.HBM) if i >= len(args) - hbm else a
        for i, a in enumerate(args)
    ]
    scratch = list(scratch) + ([pltpu.SemaphoreType.DMA((16,))] if hbm else [])
    nbytes = sum(a.size * a.dtype.itemsize for a in args)
    return pl.pallas_call(
        body,
        out_shape=outs,
        in_specs=specs,
        out_specs=jax.tree.map(
            lambda o: pl.BlockSpec(memory_space=pltpu.MemorySpace.HBM) if isinstance(o, HELD) else vmem,
            outs,
        ),
        scratch_shapes=scratch,
        compiler_params=pltpu.CompilerParams(vmem_limit_bytes=16 * 2**20),
        cost_estimate=pl.CostEstimate(flops=flops, bytes_accessed=nbytes, transcendentals=0),
    )(*args)


def local(
    fields, proj_x, proj_z, proj_bc, proj_dt, conv_x, conv_bc, dt_bias, log_rate, norm_gain, proj_out
):
    rows, _, depth = fields.shape
    heads = log_rate.shape[0]
    width = proj_x.shape[1]
    state = proj_bc.shape[1] // 2
    n_x = lax.axis_size("x")
    n_z, n_y = lax.axis_size("z"), lax.axis_size("y")
    bands = n_z * n_y
    f = fields.reshape(rows, depth)
    sds = jax.ShapeDtypeStruct

    k = proj_x.shape[0]
    x_at, c_at = lax.axis_index("x"), lax.axis_index("c")
    each = jnp.arange(2 * n_x)
    order = each % n_x * 2 + (c_at + each // n_x) % 2
    order2 = (x_at - each + 2 * n_x) % n_x * 2 + (c_at + each // n_x) % 2
    first, tail = call(
        pack_kernel,
        (sds((n_x, k + 2 * k * LANES // width, width), BF16), sds((HALO, depth), BF16)),
        [proj_x, proj_bc, proj_dt.T, f],
        hbm=4,
        scratch=[
            pltpu.VMEM(proj_x.shape, BF16),
            pltpu.VMEM(proj_bc.shape, BF16),
            pltpu.VMEM(proj_dt.shape[::-1], BF16),
        ],
    )

    def across(block):
        return lax.ppermute(block, "c", [(0, 1), (1, 0)])

    w1a = lax.all_to_all(first, "x", 0, 0)
    halo = lax.ppermute(tail, LAT, [(i, i + 1) for i in range(bands - 1)])
    small = [conv_x, conv_bc, dt_bias[None], log_rate[None]]
    src, second, f, *small = call(
        source_kernel,
        [sds((HALO + rows, depth), BF16), sds((2 * k, width), BF16), sds((rows, depth), BF16)]
        + [sds(a.shape, F32) for a in small],
        [order, halo, proj_z, proj_out, f, *small],
        smem=1,
        hbm=7,
        flops=10**6,
    )
    w2a, w2b = [second], [across(second)]
    w1a, src, second, order2, w2b[0] = lax.optimization_barrier(
        (w1a, src, second, order2, w2b[0])
    )
    w1b = across(w1a)
    for d in range(1, n_x):
        w2a.append(lax.ppermute(second, "x", [(i, (i + d) % n_x) for i in range(n_x)]))
    size = (n_x - 1) * 2 * k
    mine = call(
        stack_kernel,
        pltpu.HBM((size, width), BF16),
        w2a[1:],
        scratch=[pltpu.SemaphoreType.DMA((n_x - 1,))],
        flops=10**6,
    )
    others = across(mine)

    x_act, bc_act, step, cum, msg = call(
        project_kernel,
        (
            sds((rows, width), BF16),
            sds((rows, 2 * state), BF16),
            sds((rows, heads), F32),
            sds((rows, heads), F32),
            sds((n_y, width // heads + SUB, LANES), BF16),
        ),
        [src, w1a, w1b, *small],
        scratch=[pltpu.VMEM((HALO + rows, width + 2 * state), F32)],
        flops=2 * rows * depth * (width + 2 * LANES),
    )
    got = lax.all_to_all(msg, "y", 0, 0)
    y = call(
        within_kernel,
        sds((rows, width), F32),
        [x_act, bc_act, step, cum],
        flops=2 * rows * rows * width * 2,
    )
    per = width // heads
    before, decay, msg = call(
        row_kernel,
        (
            sds((n_y, per, LANES), F32),
            sds((n_y, LANES), F32),
            sds((n_z, per + SUB, LANES), BF16),
        ),
        [got],
        flops=10**6,
    )
    got = lax.all_to_all(msg, "z", 0, 0)
    entering = call(
        enter_kernel,
        sds((n_y, per, LANES), BF16),
        [lax.axis_index("z")[None], got, before, decay],
        smem=1,
        flops=10**6,
    )
    incoming = lax.all_to_all(entering, "y", 0, 0)
    incoming = incoming.reshape(width // 2, LANES)
    gate, w_out = call(
        gate_kernel,
        (sds((rows, width), BF16), sds((width, depth), BF16)),
        [order2, f, proj_z, proj_out, mine, w2b[0], others],
        smem=1,
        hbm=5,
        scratch=[pltpu.VMEM((depth, width), BF16)],
        flops=2 * rows * depth * width,
    )
    out = call(
        finish_kernel,
        sds((rows, depth), BF16),
        [order2, y, incoming, bc_act, cum, gate, norm_gain[None], w_out],
        smem=1,
        scratch=[pltpu.VMEM((rows, width), BF16)],
        flops=2 * rows * depth * width,
    )
    return out.reshape(rows, 1, depth)


def solution(mesh):
    finer = Mesh(mesh.devices.reshape(8, 8, 4, 2), ("z", "y", "x", "c"))
    lat, lon = P(LAT, ("x", "c"), None), P(("x", "c"), None)
    return jax.shard_map(
        local,
        mesh=finer,
        in_specs=(lat, lon, lon, lon, lon, P(), P(), P(), P(), P(), lon),
        out_specs=lat,
        check_vma=False,
    )
```

```python
import jax
import jax.numpy as jnp
from jax import lax
from jax.experimental import pallas as pl
from jax.experimental.pallas import tpu as pltpu
from jax.sharding import Mesh
from jax.sharding import PartitionSpec as P


LAT = ("z", "y")
EPS = 1e-05
HIGHEST = lax.Precision.HIGHEST
F32 = jnp.float32
BF16 = jnp.bfloat16
HALO = 16
LANES = 128
SUB = 8
TILE = 256
HELD = type(pltpu.HBM((8, 128), jnp.bfloat16))


def dot(a, b, **kw):
    return jnp.dot(a, b, preferred_element_type=F32, **kw)


def dot_nt(a, b):
    return lax.dot_general(a, b, (((1,), (1,)), ((), ())), preferred_element_type=F32)


def dot_tn(a, b):
    return lax.dot_general(a, b, (((0,), (0,)), ((), ())), preferred_element_type=F32)


def iota(shape, dim):
    return lax.broadcasted_iota(jnp.int32, shape, dim)


def silu(v):
    return v / (1.0 + jnp.exp(-v))


def halves(v):
    high = v.astype(BF16)
    return high, (v - high.astype(F32)).astype(BF16)


def spread(v, width):
    heads = v.shape[1]
    shape = (heads, width)
    pick = (iota(shape, 1) // (width // heads) == iota(shape, 0)).astype(BF16)
    high, low = halves(v)
    return dot(high, pick) + dot(low, pick)


def chunk(ref, index):
    return ref[:, pl.ds(pl.multiple_of(index * LANES, LANES), LANES)]


def ordered(ref, order, n):
    return jnp.concatenate([chunk(ref, order[j]) for j in range(n)], 1)


def stacked(refs, rows, columns):
    return jnp.concatenate([r[rows, columns] for r in refs], 0)


def fetch(pairs, sems):
    copies = [pltpu.make_async_copy(a, b, sems.at[i]) for i, (a, b) in enumerate(pairs)]
    for c in copies:
        c.start()
    return copies


def pack_kernel(x_ref, bc_ref, dt_ref, f_ref, first, tail, x, bc, dt, sems):
    k, width = x_ref.shape
    blocks = width // LANES
    part = k // blocks
    copies = fetch(
        [(x_ref, x), (bc_ref, bc), (dt_ref, dt), (f_ref.at[f_ref.shape[0] - HALO :], tail)], sems
    )
    for c in copies:
        c.wait()
    rest = jnp.zeros((part, width - LANES), BF16)
    for i in range(first.shape[0]):
        first[i, :k, :] = x[...]
        for j in range(blocks):
            first[i, k : k + part, j * LANES : (j + 1) * LANES] = bc[j * part : (j + 1) * part, :]
        first[i, k + part :, :LANES] = dt[...]
        first[i, k + part :, LANES:] = rest


def source_kernel(order, halo_ref, *refs):
    z_ref, o_ref, f_ref = refs[:3]
    small_refs = refs[3:7]
    out, second = refs[7:9]
    small, fields, sems = refs[9:13], refs[13], refs[14]
    k = z_ref.shape[0]
    copies = fetch(
        [(f_ref, fields), (z_ref, second.at[:k]), (o_ref, second.at[k:])]
        + list(zip(small_refs, small)),
        sems,
    )
    n = out.shape[1] // LANES
    copies[0].wait()
    for j in range(n):
        at = slice(j * LANES, (j + 1) * LANES)
        out[:HALO, at] = chunk(halo_ref, order[j])
        out[HALO:, at] = chunk(fields, order[j])
    for c in copies[1:]:
        c.wait()


def tail_rows(high, low):
    row = iota((SUB, LANES), 0)
    return jnp.where(row == 0, high, jnp.where(row == 1, low, 0.0)).astype(BF16)


def part_of(ref, b):
    size = ref.shape[1] - SUB
    tail = ref[b, size:, :].astype(F32)
    return ref[b, :size, :].astype(F32), tail[0:1, :] + tail[1:2, :]


def project_kernel(
    src_ref, wa, wb, conv_x, conv_bc, bias, rate, x_out, bc_out, dt_out, cum_out, msg_out, pre
):
    rows, width = x_out.shape
    heads = bias.shape[1]
    per = width // heads
    half = width // 2
    k = LANES
    n = 2 * wa.shape[0]
    blocks = width // LANES
    part = k // blocks
    shards = [r.at[i] for r in (wa, wb) for i in range(n // 2)]
    src = src_ref[...]
    first = HALO - conv_x.shape[0] + 1

    def conv(at, wide, taps):
        acc = taps[0:1, :] * pre[first : first + rows, at : at + wide]
        for i in range(1, conv_x.shape[0]):
            acc = acc + taps[i : i + 1, :] * pre[first + i : first + i + rows, at : at + wide]
        return silu(acc)

    w_dt = jnp.concatenate([r[i, k + part :, :LANES] for r in (wa, wb) for i in range(n // 2)], 1)
    dt_pre = dot_nt(src[HALO:], w_dt).astype(BF16).astype(F32)
    step = jax.nn.softplus(dt_pre + bias[...])
    log_step = -jnp.exp(rate[...]) * step
    lower = (iota((rows, rows), 0) >= iota((rows, rows), 1)).astype(F32)
    cum = dot(lower, log_step, precision=HIGHEST)
    dt_out[...] = step.T
    cum_out[...] = cum.T
    last = cum[rows - 1 : rows, :]
    weight = spread(jnp.exp(last - cum) * step, width)

    w_bc = jnp.concatenate(
        [
            r[i, k : k + part, j * LANES : (j + 1) * LANES]
            for r in (wa, wb)
            for i in range(n // 2)
            for j in range(blocks)
        ],
        0,
    )
    pre[:, width:] = dot(src, w_bc).astype(BF16).astype(F32)
    bc = conv(width, LANES, conv_bc[...])
    bc_out[...] = bc.astype(BF16)
    left = iota((rows, LANES), 1) < LANES // 2
    b0 = jnp.where(left, bc, 0.0)
    b = (b0.astype(BF16), pltpu.roll(b0, LANES // 2, 1).astype(BF16))

    def end(at, q):
        pre[:, at : at + TILE] = (
            dot(src, stacked(shards, slice(0, k), slice(at, at + TILE))).astype(BF16).astype(F32)
        )
        x = conv(at, TILE, conv_x[:, at : at + TILE]).astype(BF16)
        x_out[:, at : at + TILE] = x
        xw = (x.astype(F32) * weight[:, at : at + TILE]).astype(BF16)
        return dot_tn(xw, b[q])

    for at in range(0, half, TILE):
        t = end(at, 0) + end(half + at, 1)
        for i in range(0, TILE, per):
            msg_out[(at + i) // per, :per, :] = t[i : i + per].astype(BF16)
    pairs = heads // 2
    mine = iota((pairs, heads), 1) % pairs == iota((pairs, heads), 0)
    pick = (iota((heads, LANES), 1) // (LANES // 2) == iota((heads, LANES), 0) // pairs).astype(BF16)
    high, low = (dot(jnp.where(mine, v.astype(F32), 0.0).astype(BF16), pick) for v in halves(last))
    for j in range(pairs):
        msg_out[j, per:, :] = tail_rows(high[j : j + 1, :], low[j : j + 1, :])


def within_kernel(x_ref, bc_ref, dt_ref, cum_ref, y_out):
    rows, _ = x_ref.shape
    heads = dt_ref.shape[0]
    state = bc_ref.shape[1] // 2
    scores = dot_nt(bc_ref[:, state:], bc_ref[:, :state])
    causal = iota((rows, rows), 0) >= iota((rows, rows), 1)
    cum_t = cum_ref[...]
    cum = cum_t.T
    dt_t = dt_ref[...]
    left = iota((rows, LANES), 1) < LANES // 2
    for pair in range(heads // 2):
        w = []
        for h in (2 * pair, 2 * pair + 1):
            gap = jnp.where(causal, cum[:, h : h + 1] - cum_t[h : h + 1, :], -jnp.inf)
            w.append((jnp.exp(gap) * (scores * dt_t[h : h + 1, :])).astype(BF16))
        xp = x_ref[:, pair * LANES : (pair + 1) * LANES]
        zero = jnp.zeros_like(xp)
        both = jnp.concatenate([jnp.where(left, xp, zero), jnp.where(left, zero, xp)], 0)
        y_out[:, pair * LANES : (pair + 1) * LANES] = dot(jnp.concatenate(w, 1), both)


def stack_kernel(*refs):
    parts, (out, sems) = refs[:-2], refs[-2:]
    size = parts[0].shape[0]
    for c in fetch([(r, out.at[pl.ds(i * size, size)]) for i, r in enumerate(parts)], sems):
        c.wait()


def row_kernel(r_ref, before, decay, msg_out):
    state = jnp.zeros(before.shape[1:], F32)
    total = jnp.zeros((1, LANES), F32)
    for b in range(r_ref.shape[0]):
        before[b] = state
        decay[b : b + 1, :] = total
        own, step = part_of(r_ref, b)
        state = jnp.exp(step) * state + own
        total = total + step
    high, low = (v.astype(F32) for v in halves(total))
    tail = tail_rows(high, low)
    for z in range(msg_out.shape[0]):
        msg_out[z, : state.shape[0], :] = state.astype(BF16)
        msg_out[z, state.shape[0] :, :] = tail


def enter_kernel(place, r_ref, before, decay, e_out):
    state = jnp.zeros(before.shape[1:], F32)
    for z in range(r_ref.shape[0]):
        own, step = part_of(r_ref, z)
        state = jnp.where(z < place[0], jnp.exp(step) * state + own, state)
    for b in range(e_out.shape[0]):
        e_out[b] = (before[b] + jnp.exp(decay[b : b + 1, :]) * state).astype(BF16)


def gate_kernel(order, f_ref, z_ref, o_ref, mine, other, others, out, w_out, w, fields, sems):
    k, width = z_ref.shape
    n = w.shape[0] // k
    shards = [(z_ref, o_ref)]
    for ref in (mine, other, others):
        for i in range(0, ref.shape[0], 2 * k):
            shards.append((ref.at[pl.ds(i, k)], ref.at[pl.ds(i + k, k)]))
    copies = fetch(
        [(f_ref, fields)]
        + [(s[0], w.at[pl.ds(i * k, k)]) for i, s in enumerate(shards)]
        + [(s[1], w_out.at[pl.ds(i * k, k)]) for i, s in enumerate(shards)],
        sems,
    )
    for c in copies[: n + 1]:
        c.wait()
    src = ordered(fields, order, n)
    for at in range(0, width, TILE):
        out[:, at : at + TILE] = dot(src, w[:, at : at + TILE]).astype(BF16)
    for c in copies[n + 1 :]:
        c.wait()


def finish_kernel(order, y_ref, in_ref, bc_ref, cum_ref, gate_ref, gain, w, out, hidden):
    rows, width = y_ref.shape
    half = width // 2
    bc = bc_ref[...].astype(F32)
    left = iota((rows, LANES), 1) < LANES // 2
    c1 = jnp.where(left, 0.0, bc)
    c = (pltpu.roll(c1, LANES // 2, 1).astype(BF16), c1.astype(BF16))
    grown = spread(jnp.exp(cum_ref[...]).T, width)
    square = jnp.zeros((rows, 1), F32)
    parts = []
    for at in range(0, width, TILE):
        inner = in_ref[at % half : at % half + TILE, :]
        y = y_ref[:, at : at + TILE] + dot_nt(c[at // half], inner) * grown[:, at : at + TILE]
        g = y * silu(gate_ref[:, at : at + TILE].astype(F32))
        square = square + jnp.sum(g * g, -1, keepdims=True)
        parts.append(g)
    scale = lax.rsqrt(square / width + EPS)
    for i, at in enumerate(range(0, width, TILE)):
        hidden[:, at : at + TILE] = (parts[i] * scale * gain[:, at : at + TILE]).astype(BF16)
    src = ordered(hidden, order, width // LANES)
    for at in range(0, out.shape[1], TILE):
        out[:, at : at + TILE] = dot(src, w[:, at : at + TILE]).astype(BF16)


def call(body, outs, args, smem=0, hbm=0, scratch=(), flops=0):
    vmem = pl.BlockSpec(memory_space=pltpu.VMEM)
    specs = (
        [pl.BlockSpec(memory_space=pltpu.SMEM)] * smem
        + [vmem] * (len(args) - smem - hbm)
        + [pl.BlockSpec(memory_space=pltpu.MemorySpace.HBM)] * hbm
    )
    args = [
        pltpu.with_memory_space_constraint(a, pltpu.MemorySpace.HBM) if i >= len(args) - hbm else a
        for i, a in enumerate(args)
    ]
    scratch = list(scratch) + ([pltpu.SemaphoreType.DMA((24,))] if hbm else [])
    nbytes = sum(a.size * a.dtype.itemsize for a in args)
    return pl.pallas_call(
        body,
        out_shape=outs,
        in_specs=specs,
        out_specs=jax.tree.map(
            lambda o: pl.BlockSpec(memory_space=pltpu.MemorySpace.HBM) if isinstance(o, HELD) else vmem,
            outs,
        ),
        scratch_shapes=scratch,
        compiler_params=pltpu.CompilerParams(vmem_limit_bytes=16 * 2**20),
        cost_estimate=pl.CostEstimate(flops=flops, bytes_accessed=nbytes, transcendentals=0),
    )(*args)


def local(
    fields, proj_x, proj_z, proj_bc, proj_dt, conv_x, conv_bc, dt_bias, log_rate, norm_gain, proj_out
):
    rows, _, depth = fields.shape
    heads = log_rate.shape[0]
    width = proj_x.shape[1]
    state = proj_bc.shape[1] // 2
    n_x = lax.axis_size("x")
    n_z, n_y = lax.axis_size("z"), lax.axis_size("y")
    bands = n_z * n_y
    f = fields.reshape(rows, depth)
    sds = jax.ShapeDtypeStruct

    k = proj_x.shape[0]
    x_at, c_at = lax.axis_index("x"), lax.axis_index("c")
    each = jnp.arange(2 * n_x)
    order = each % n_x * 2 + (c_at + each // n_x) % 2
    order2 = (x_at - each + 2 * n_x) % n_x * 2 + (c_at + each // n_x) % 2
    first, tail = call(
        pack_kernel,
        (sds((n_x, k + 2 * k * LANES // width, width), BF16), sds((HALO, depth), BF16)),
        [proj_x, proj_bc, proj_dt.T, f],
        hbm=4,
        scratch=[
            pltpu.VMEM(proj_x.shape, BF16),
            pltpu.VMEM(proj_bc.shape, BF16),
            pltpu.VMEM(proj_dt.shape[::-1], BF16),
        ],
    )

    def across(block):
        return lax.ppermute(block, "c", [(0, 1), (1, 0)])

    w1a = lax.all_to_all(first, "x", 0, 0)
    halo = lax.ppermute(tail, LAT, [(i, i + 1) for i in range(bands - 1)])
    small = [conv_x, conv_bc, dt_bias[None], log_rate[None]]
    src, second, *small = call(
        source_kernel,
        [sds((HALO + rows, depth), BF16), sds((2 * k, width), BF16)]
        + [sds(a.shape, F32) for a in small],
        [order, halo, proj_z, proj_out, f, *small],
        smem=1,
        hbm=7,
        scratch=[pltpu.VMEM((rows, depth), BF16)],
        flops=10**6,
    )
    w2a, w2b = [second], [across(second)]
    w1a, src, second, order2, w2b[0] = lax.optimization_barrier(
        (w1a, src, second, order2, w2b[0])
    )
    w1b = across(w1a)
    for d in range(1, n_x):
        w2a.append(lax.ppermute(second, "x", [(i, (i + d) % n_x) for i in range(n_x)]))
    size = (n_x - 1) * 2 * k
    mine = call(
        stack_kernel,
        pltpu.HBM((size, width), BF16),
        w2a[1:],
        scratch=[pltpu.SemaphoreType.DMA((n_x - 1,))],
        flops=10**6,
    )
    others = across(mine)

    x_act, bc_act, step, cum, msg = call(
        project_kernel,
        (
            sds((rows, width), BF16),
            sds((rows, 2 * state), BF16),
            sds((heads, rows), F32),
            sds((heads, rows), F32),
            sds((n_y, width // heads + SUB, LANES), BF16),
        ),
        [src, w1a, w1b, *small],
        scratch=[pltpu.VMEM((HALO + rows, width + 2 * state), F32)],
        flops=2 * rows * depth * (width + 2 * LANES),
    )
    got = lax.all_to_all(msg, "y", 0, 0)
    y = call(
        within_kernel,
        sds((rows, width), F32),
        [x_act, bc_act, step, cum],
        flops=2 * rows * rows * width * 2,
    )
    per = width // heads
    before, decay, msg = call(
        row_kernel,
        (
            sds((n_y, per, LANES), F32),
            sds((n_y, LANES), F32),
            sds((n_z, per + SUB, LANES), BF16),
        ),
        [got],
        flops=10**6,
    )
    got = lax.all_to_all(msg, "z", 0, 0)
    entering = call(
        enter_kernel,
        sds((n_y, per, LANES), BF16),
        [lax.axis_index("z")[None], got, before, decay],
        smem=1,
        flops=10**6,
    )
    incoming = lax.all_to_all(entering, "y", 0, 0)
    incoming = incoming.reshape(width // 2, LANES)
    gate, w_out = call(
        gate_kernel,
        (sds((rows, width), BF16), sds((width, depth), BF16)),
        [order2, f, proj_z, proj_out, mine, w2b[0], others],
        smem=1,
        hbm=6,
        scratch=[pltpu.VMEM((depth, width), BF16), pltpu.VMEM((rows, depth), BF16)],
        flops=2 * rows * depth * width,
    )
    out = call(
        finish_kernel,
        sds((rows, depth), BF16),
        [order2, y, incoming, bc_act, cum, gate, norm_gain[None], w_out],
        smem=1,
        scratch=[pltpu.VMEM((rows, width), BF16)],
        flops=2 * rows * depth * width,
    )
    return out.reshape(rows, 1, depth)


def solution(mesh):
    finer = Mesh(mesh.devices.reshape(8, 8, 4, 2), ("z", "y", "x", "c"))
    lat, lon = P(LAT, ("x", "c"), None), P(("x", "c"), None)
    return jax.shard_map(
        local,
        mesh=finer,
        in_specs=(lat, lon, lon, lon, lon, P(), P(), P(), P(), P(), lon),
        out_specs=lat,
        check_vma=False,
    )
```

```python
import functools

import jax
import jax.numpy as jnp
from jax import lax
from jax.experimental import pallas as pl
from jax.experimental.pallas import tpu as pltpu
from jax.sharding import Mesh
from jax.sharding import PartitionSpec as P


LAT = ("z", "y")
EPS = 1e-05
HIGHEST = lax.Precision.HIGHEST
F32 = jnp.float32
BF16 = jnp.bfloat16
HALO = 16
LANES = 128
SUB = 8
TILE = 256


def dot(a, b, **kw):
    return jnp.dot(a, b, preferred_element_type=F32, **kw)


def dot_nt(a, b):
    return lax.dot_general(a, b, (((1,), (1,)), ((), ())), preferred_element_type=F32)


def dot_tn(a, b):
    return lax.dot_general(a, b, (((0,), (0,)), ((), ())), preferred_element_type=F32)


def iota(shape, dim):
    return lax.broadcasted_iota(jnp.int32, shape, dim)


def silu(v):
    return v / (1.0 + jnp.exp(-v))


def halves(v):
    high = v.astype(BF16)
    return high, (v - high.astype(F32)).astype(BF16)


def spread(v, width):
    heads = v.shape[1]
    shape = (heads, width)
    pick = (iota(shape, 1) // (width // heads) == iota(shape, 0)).astype(BF16)
    high, low = halves(v)
    return dot(high, pick) + dot(low, pick)


def chunk(ref, index):
    return ref[:, pl.ds(pl.multiple_of(index * LANES, LANES), LANES)]


def ordered(ref, order, n):
    return jnp.concatenate([chunk(ref, order[j]) for j in range(n)], 1)


def stacked(refs, rows, columns):
    return jnp.concatenate([r[rows, columns] for r in refs], 0)


def fetch(pairs, sems):
    copies = [pltpu.make_async_copy(a, b, sems.at[i]) for i, (a, b) in enumerate(pairs)]
    for c in copies:
        c.start()
    return copies


def pack_kernel(x_ref, bc_ref, dt_ref, f_ref, first, tail, x, bc, dt, sems):
    k, width = x_ref.shape
    blocks = width // LANES
    part = k // blocks
    copies = fetch(
        [(x_ref, x), (bc_ref, bc), (dt_ref, dt), (f_ref.at[f_ref.shape[0] - HALO :], tail)], sems
    )
    for c in copies:
        c.wait()
    rest = jnp.zeros((part, width - LANES), BF16)
    for i in range(first.shape[0]):
        first[i, :k, :] = x[...]
        for j in range(blocks):
            first[i, k : k + part, j * LANES : (j + 1) * LANES] = bc[j * part : (j + 1) * part, :]
        first[i, k + part :, :LANES] = dt[...]
        first[i, k + part :, LANES:] = rest


def source_kernel(order, halo_ref, *refs):
    z_ref, o_ref, f_ref = refs[:3]
    small_refs = refs[3:7]
    out, second, fields = refs[7:10]
    small, sems = refs[10:14], refs[14]
    k = z_ref.shape[0]
    copies = fetch(
        [(f_ref, fields), (z_ref, second.at[:k]), (o_ref, second.at[k:])]
        + list(zip(small_refs, small)),
        sems,
    )
    n = out.shape[1] // LANES
    copies[0].wait()
    for j in range(n):
        at = slice(j * LANES, (j + 1) * LANES)
        out[:HALO, at] = chunk(halo_ref, order[j])
        out[HALO:, at] = chunk(fields, order[j])
    for c in copies[1:]:
        c.wait()


def tail_rows(high, low):
    row = iota((SUB, LANES), 0)
    return jnp.where(row == 0, high, jnp.where(row == 1, low, 0.0)).astype(BF16)


def part_of(ref, b):
    size = ref.shape[1] - SUB
    tail = ref[b, size:, :].astype(F32)
    return ref[b, :size, :].astype(F32), tail[0:1, :] + tail[1:2, :]


def project_kernel(
    src_ref, wa, wb, conv_x, conv_bc, bias, rate, x_out, bc_out, dt_out, cum_out, msg_out, pre
):
    rows, width = x_out.shape
    heads = bias.shape[1]
    per = width // heads
    half = width // 2
    k = LANES
    n = 2 * wa.shape[0]
    blocks = width // LANES
    part = k // blocks
    shards = [r.at[i] for r in (wa, wb) for i in range(n // 2)]
    src = src_ref[...]
    first = HALO - conv_x.shape[0] + 1

    def conv(at, wide, taps):
        acc = taps[0:1, :] * pre[first : first + rows, at : at + wide]
        for i in range(1, conv_x.shape[0]):
            acc = acc + taps[i : i + 1, :] * pre[first + i : first + i + rows, at : at + wide]
        return silu(acc)

    w_dt = jnp.concatenate([r[i, k + part :, :LANES] for r in (wa, wb) for i in range(n // 2)], 1)
    dt_pre = dot_nt(src[HALO:], w_dt).astype(BF16).astype(F32)
    step = jax.nn.softplus(dt_pre + bias[...])
    log_step = -jnp.exp(rate[...]) * step
    lower = (iota((rows, rows), 0) >= iota((rows, rows), 1)).astype(F32)
    cum = dot(lower, log_step, precision=HIGHEST)
    dt_out[...] = step.T
    cum_out[...] = cum.T
    last = cum[rows - 1 : rows, :]
    weight = spread(jnp.exp(last - cum) * step, width)

    w_bc = jnp.concatenate(
        [
            r[i, k : k + part, j * LANES : (j + 1) * LANES]
            for r in (wa, wb)
            for i in range(n // 2)
            for j in range(blocks)
        ],
        0,
    )
    pre[:, width:] = dot(src, w_bc).astype(BF16).astype(F32)
    bc = conv(width, LANES, conv_bc[...])
    bc_out[...] = bc.astype(BF16)
    left = iota((rows, LANES), 1) < LANES // 2
    b0 = jnp.where(left, bc, 0.0)
    b = (b0.astype(BF16), pltpu.roll(b0, LANES // 2, 1).astype(BF16))

    def end(at, q):
        pre[:, at : at + TILE] = (
            dot(src, stacked(shards, slice(0, k), slice(at, at + TILE))).astype(BF16).astype(F32)
        )
        x = conv(at, TILE, conv_x[:, at : at + TILE]).astype(BF16)
        x_out[:, at : at + TILE] = x
        xw = (x.astype(F32) * weight[:, at : at + TILE]).astype(BF16)
        return dot_tn(xw, b[q])

    for at in range(0, half, TILE):
        t = end(at, 0) + end(half + at, 1)
        for i in range(0, TILE, per):
            msg_out[(at + i) // per, :per, :] = t[i : i + per].astype(BF16)
    pairs = heads // 2
    mine = iota((pairs, heads), 1) % pairs == iota((pairs, heads), 0)
    pick = (iota((heads, LANES), 1) // (LANES // 2) == iota((heads, LANES), 0) // pairs).astype(BF16)
    high, low = (dot(jnp.where(mine, v.astype(F32), 0.0).astype(BF16), pick) for v in halves(last))
    for j in range(pairs):
        msg_out[j, per:, :] = tail_rows(high[j : j + 1, :], low[j : j + 1, :])


def within_kernel(x_ref, bc_ref, dt_ref, cum_ref, y_out):
    rows, _ = x_ref.shape
    heads = dt_ref.shape[0]
    state = bc_ref.shape[1] // 2
    scores = dot_nt(bc_ref[:, state:], bc_ref[:, :state])
    causal = iota((rows, rows), 0) >= iota((rows, rows), 1)
    cum_t = cum_ref[...]
    cum = cum_t.T
    dt_t = dt_ref[...]
    left = iota((rows, LANES), 1) < LANES // 2
    for pair in range(heads // 2):
        w = []
        for h in (2 * pair, 2 * pair + 1):
            gap = jnp.where(causal, cum[:, h : h + 1] - cum_t[h : h + 1, :], -jnp.inf)
            w.append((jnp.exp(gap) * (scores * dt_t[h : h + 1, :])).astype(BF16))
        xp = x_ref[:, pair * LANES : (pair + 1) * LANES]
        zero = jnp.zeros_like(xp)
        both = jnp.concatenate([jnp.where(left, xp, zero), jnp.where(left, zero, xp)], 0)
        y_out[:, pair * LANES : (pair + 1) * LANES] = dot(jnp.concatenate(w, 1), both)


def row_kernel(r_ref, before, decay, msg_out):
    state = jnp.zeros(before.shape[1:], F32)
    total = jnp.zeros((1, LANES), F32)
    for b in range(r_ref.shape[0]):
        before[b] = state
        decay[b : b + 1, :] = total
        own, step = part_of(r_ref, b)
        state = jnp.exp(step) * state + own
        total = total + step
    high, low = (v.astype(F32) for v in halves(total))
    tail = tail_rows(high, low)
    for z in range(msg_out.shape[0]):
        msg_out[z, : state.shape[0], :] = state.astype(BF16)
        msg_out[z, state.shape[0] :, :] = tail


def enter_kernel(place, r_ref, before, decay, e_out):
    state = jnp.zeros(before.shape[1:], F32)
    for z in range(r_ref.shape[0]):
        own, step = part_of(r_ref, z)
        state = jnp.where(z < place[0], jnp.exp(step) * state + own, state)
    for b in range(e_out.shape[0]):
        e_out[b] = (before[b] + jnp.exp(decay[b : b + 1, :]) * state).astype(BF16)


def gate_kernel(near, order, f_ref, *refs):
    (out, w_out, w, sems) = refs[-4:]
    near_refs, (z_ref, o_ref), far_refs = refs[:near], refs[near : near + 2], refs[near + 2 : -4]
    k = z_ref.shape[0]
    n = len(far_refs) + 1 + near
    at = [pl.ds(i * k, k) for i in range(n)]
    copies = fetch(
        [(z_ref, w.at[at[0]])]
        + [(r.at[:k], w.at[at[i]]) for i, r in enumerate(far_refs, 1)]
        + [(o_ref, w_out.at[at[0]])]
        + [(r.at[k:], w_out.at[at[i]]) for i, r in enumerate(far_refs, 1)],
        sems,
    )
    for i, r in enumerate(near_refs, n - near):
        w_out[i * k : (i + 1) * k, :] = r[k:, :]
    src = ordered(f_ref, order, n)
    for c in copies[: n - near]:
        c.wait()
    for j in range(0, out.shape[1], TILE):
        cut = slice(j, j + TILE)
        tile = jnp.concatenate([w[: (n - near) * k, cut]] + [r[:k, cut] for r in near_refs], 0)
        out[:, cut] = dot(src, tile).astype(BF16)
    for c in copies[n - near :]:
        c.wait()


def finish_kernel(order, y_ref, in_ref, bc_ref, cum_ref, gate_ref, gain, w, out, hidden):
    rows, width = y_ref.shape
    half = width // 2
    bc = bc_ref[...].astype(F32)
    left = iota((rows, LANES), 1) < LANES // 2
    c1 = jnp.where(left, 0.0, bc)
    c = (pltpu.roll(c1, LANES // 2, 1).astype(BF16), c1.astype(BF16))
    grown = spread(jnp.exp(cum_ref[...]).T, width)
    square = jnp.zeros((rows, 1), F32)
    parts = []
    for at in range(0, width, TILE):
        inner = in_ref[at % half : at % half + TILE, :]
        y = y_ref[:, at : at + TILE] + dot_nt(c[at // half], inner) * grown[:, at : at + TILE]
        g = y * silu(gate_ref[:, at : at + TILE].astype(F32))
        square = square + jnp.sum(g * g, -1, keepdims=True)
        parts.append(g)
    scale = lax.rsqrt(square / width + EPS)
    for i, at in enumerate(range(0, width, TILE)):
        hidden[:, at : at + TILE] = (parts[i] * scale * gain[:, at : at + TILE]).astype(BF16)
    src = ordered(hidden, order, width // LANES)
    for at in range(0, out.shape[1], TILE):
        out[:, at : at + TILE] = dot(src, w[:, at : at + TILE]).astype(BF16)


def call(body, outs, args, smem=0, hbm=0, scratch=(), flops=0):
    vmem = pl.BlockSpec(memory_space=pltpu.VMEM)
    specs = (
        [pl.BlockSpec(memory_space=pltpu.SMEM)] * smem
        + [vmem] * (len(args) - smem - hbm)
        + [pl.BlockSpec(memory_space=pltpu.MemorySpace.HBM)] * hbm
    )
    args = [
        pltpu.with_memory_space_constraint(a, pltpu.MemorySpace.HBM) if i >= len(args) - hbm else a
        for i, a in enumerate(args)
    ]
    scratch = list(scratch) + ([pltpu.SemaphoreType.DMA((2 * hbm,))] if hbm else [])
    nbytes = sum(a.size * a.dtype.itemsize for a in args)
    return pl.pallas_call(
        body,
        out_shape=outs,
        in_specs=specs,
        out_specs=jax.tree.map(lambda _: vmem, outs),
        scratch_shapes=scratch,
        compiler_params=pltpu.CompilerParams(vmem_limit_bytes=16 * 2**20),
        cost_estimate=pl.CostEstimate(flops=flops, bytes_accessed=nbytes, transcendentals=0),
    )(*args)


def local(
    fields, proj_x, proj_z, proj_bc, proj_dt, conv_x, conv_bc, dt_bias, log_rate, norm_gain, proj_out
):
    rows, _, depth = fields.shape
    heads = log_rate.shape[0]
    width = proj_x.shape[1]
    state = proj_bc.shape[1] // 2
    n_x = lax.axis_size("x")
    n_z, n_y = lax.axis_size("z"), lax.axis_size("y")
    bands = n_z * n_y
    f = fields.reshape(rows, depth)
    sds = jax.ShapeDtypeStruct

    k = proj_x.shape[0]
    x_at, c_at = lax.axis_index("x"), lax.axis_index("c")
    each = jnp.arange(2 * n_x)
    order = each % n_x * 2 + (c_at + each // n_x) % 2
    late = jnp.array([0, 1, 3, 2, 4, 6, 5, 7])
    order2 = (x_at - late + 2 * n_x) % n_x * 2 + (c_at + late // n_x) % 2
    first, tail = call(
        pack_kernel,
        (sds((n_x, k + 2 * k * LANES // width, width), BF16), sds((HALO, depth), BF16)),
        [proj_x, proj_bc, proj_dt.T, f],
        hbm=4,
        scratch=[
            pltpu.VMEM(proj_x.shape, BF16),
            pltpu.VMEM(proj_bc.shape, BF16),
            pltpu.VMEM(proj_dt.shape[::-1], BF16),
        ],
    )

    def across(block):
        return lax.ppermute(block, "c", [(0, 1), (1, 0)])

    w1a = lax.all_to_all(first, "x", 0, 0)
    halo = lax.ppermute(tail, LAT, [(i, i + 1) for i in range(bands - 1)])
    small = [conv_x, conv_bc, dt_bias[None], log_rate[None]]
    src, second, f, *small = call(
        source_kernel,
        [sds((HALO + rows, depth), BF16), sds((2 * k, width), BF16), sds((rows, depth), BF16)]
        + [sds(a.shape, F32) for a in small],
        [order, halo, proj_z, proj_out, f, *small],
        smem=1,
        hbm=7,
        flops=10**6,
    )
    w2a, w2b = [second], [across(second)]
    w1a, src, second, order2 = lax.optimization_barrier((w1a, src, second, order2))
    w1b = across(w1a)
    for d in range(1, n_x):
        w2a.append(lax.ppermute(second, "x", [(i, (i + d) % n_x) for i in range(n_x)]))
    for d in range(1, n_x):
        w2b.append(across(w2a[d]))

    x_act, bc_act, step, cum, msg = call(
        project_kernel,
        (
            sds((rows, width), BF16),
            sds((rows, 2 * state), BF16),
            sds((heads, rows), F32),
            sds((heads, rows), F32),
            sds((n_y, width // heads + SUB, LANES), BF16),
        ),
        [src, w1a, w1b, *small],
        scratch=[pltpu.VMEM((HALO + rows, width + 2 * state), F32)],
        flops=2 * rows * depth * (width + 2 * LANES),
    )
    got = lax.all_to_all(msg, "y", 0, 0)
    y = call(
        within_kernel,
        sds((rows, width), F32),
        [x_act, bc_act, step, cum],
        flops=2 * rows * rows * width * 2,
    )
    per = width // heads
    before, decay, msg = call(
        row_kernel,
        (
            sds((n_y, per, LANES), F32),
            sds((n_y, LANES), F32),
            sds((n_z, per + SUB, LANES), BF16),
        ),
        [got],
        flops=10**6,
    )
    got = lax.all_to_all(msg, "z", 0, 0)
    entering = call(
        enter_kernel,
        sds((n_y, per, LANES), BF16),
        [lax.axis_index("z")[None], got, before, decay],
        smem=1,
        flops=10**6,
    )
    incoming = lax.all_to_all(entering, "y", 0, 0)
    incoming = incoming.reshape(width // 2, LANES)
    near = []
    gate, w_out = call(
        functools.partial(gate_kernel, len(near)),
        (sds((rows, width), BF16), sds((width, depth), BF16)),
        [order2, f, *near, proj_z, proj_out, w2a[1], w2a[3], w2a[2], w2b[0], w2b[2], w2b[1], w2b[3]],
        smem=1,
        hbm=9,
        scratch=[pltpu.VMEM((depth, width), BF16)],
        flops=2 * rows * depth * width,
    )
    out = call(
        finish_kernel,
        sds((rows, depth), BF16),
        [order2, y, incoming, bc_act, cum, gate, norm_gain[None], w_out],
        smem=1,
        scratch=[pltpu.VMEM((rows, width), BF16)],
        flops=2 * rows * depth * width,
    )
    return out.reshape(rows, 1, depth)


def solution(mesh):
    finer = Mesh(mesh.devices.reshape(8, 8, 4, 2), ("z", "y", "x", "c"))
    lat, lon = P(LAT, ("x", "c"), None), P(("x", "c"), None)
    return jax.shard_map(
        local,
        mesh=finer,
        in_specs=(lat, lon, lon, lon, lon, P(), P(), P(), P(), P(), lon),
        out_specs=lat,
        check_vma=False,
    )
```
